128 devices in a mesh: tm: 16 (over x, y), space: 8 (over z, core).
Axes of the slice: x: 4, y: 4, z: 4, core: 2. Of those that a mesh axis runs over, the one named last changes fastest.
Arguments:
- initial_state: float32 [1024, 1024], P('space'), may hold values from -6 to 6
- guess_coarse: float32 [16, 1024, 1024], P('tm', 'space'), may hold values from -6 to 6
- force_fine: float32 [16, 1024, 1024], P('tm', 'space'), may hold values from -6 to 6
- force_coarse: float32 [16, 1024, 1024], P('tm', 'space'), may hold values from -6 to 6
- eigen_basis: float32 [1024, 1024], replicated, may hold values from -1 to 1, as said below
- eigen_rates: float32 [1024], replicated, may hold values from 0.02 to 4
- carried_correction: float32 [1024, 1024], replicated, may hold values from -6 to 6
Outputs:
- fine_states: float32 [16, 1024, 1024], P('tm', 'space')
- coarse_states: float32 [16, 1024, 1024], P('tm', 'space')
The draws below stay inside these ranges and needn't reach their ends.
Inputs may be any that keep to these rules, and one draw needn't show every extreme that they name: `eigen_basis`: an orthogonal matrix: its transpose is its inverse up to float32 rounding.
All inputs are finite; a program needn't handle non-finite values.
Results may differ from the reference program's by a relative error of at most 0.00013.
Values sent between devices are 32-bit elements; how exact they have to be, the bound alone decides.
A program may use at most 64 MiB of HBM per device.

```python
import math
import jax
import jax.numpy as jnp
from jax import lax

GRID = 1024
GROUPS = 16


def draw_eigen_basis(key, part):
    skewed = jax.random.normal(key, (GRID, GRID), jnp.float32) / math.sqrt(GRID)
    skewed = skewed - skewed.T
    identity = jnp.eye(GRID, dtype=jnp.float32)
    return jnp.linalg.solve(identity + skewed, identity - skewed)


def shard_levels(stream_key, dims, split, least, high):
    level = 1.0
    for dim, shards_of in split:
        heights = jax.random.uniform(jax.random.fold_in(jax.random.fold_in(stream_key, 6), dim), (shards_of,), jnp.float32, least / len(split), high / len(split))
        level = level * jnp.repeat(jnp.exp(heights), dims[dim] // shards_of).reshape((-1,) + (1,) * (len(dims) - 1 - dim))
    return level


def scatter_about(key, shape, scale, most, pieces=(), kind=jnp.bfloat16):
    loudness = shard_levels(key, shape, pieces, -0.22, 0.18) if pieces else 1.0
    array = jax.random.normal(key, shape, jnp.float32) * scale * loudness
    return jnp.minimum(jnp.maximum(array, -most), most).astype(kind)


def setup_inputs(seed: int = 0) -> dict:
    key_of = jax.random.split(jax.random.key(seed), 8)
    return {
        "initial_state": scatter_about(key_of[0], (GRID, GRID), 1.0, 6.0, ((0, 8),), jnp.float32),
        "guess_coarse": scatter_about(key_of[1], (GROUPS, GRID, GRID), 1.0, 6.0, ((0, 16), (1, 8)), jnp.float32),
        "force_fine": scatter_about(key_of[2], (GROUPS, GRID, GRID), 1.0, 6.0, ((0, 16), (1, 8)), jnp.float32),
        "force_coarse": scatter_about(key_of[3], (GROUPS, GRID, GRID), 1.0, 6.0, ((0, 16), (1, 8)), jnp.float32),
        "eigen_basis": draw_eigen_basis(jax.random.fold_in(key_of[7], 71), 0),
        "eigen_rates": jnp.clip(jnp.exp(jax.random.uniform(key_of[5], (GRID,), jnp.float32, math.log(0.02), math.log(4.0))), 0.02, 4.0),
        "carried_correction": scatter_about(key_of[6], (GRID, GRID), 1.0, 6.0, (), jnp.float32),
    }


exact_mode = lax.Precision.HIGHEST

def reference(initial_state, guess_coarse, force_fine, force_coarse, eigen_basis, eigen_rates, carried_correction):
    fine_decay = 1.0 / (1.0 + eigen_rates[:, None] + eigen_rates[None, :])
    coarse_decay = 1.0 / (1.0 + 2.0 * (eigen_rates[:, None] + eigen_rates[None, :]))

    def to_eigen(field):
        right = jnp.einsum('gij,jk->gik', field, eigen_basis, precision=exact_mode)
        return jnp.einsum('ji,gjk->gik', eigen_basis, right, precision=exact_mode)

    def from_eigen(coeffs):
        left = jnp.einsum('ij,gjk->gik', eigen_basis, coeffs, precision=exact_mode)
        return jnp.einsum('gij,kj->gik', left, eigen_basis, precision=exact_mode)

    def reaction(field):
        return field + 0.5 * jnp.tanh(field)

    def propagate(field, source):
        return from_eigen(fine_decay[None] * to_eigen(reaction(field) + source))

    def previous(states):
        return jnp.concatenate([initial_state[None], states[:-1]], axis=0)
    relaxed_fine = propagate(previous(guess_coarse), force_fine)
    relaxed_coarse = propagate(relaxed_fine, force_coarse)
    second_fine = propagate(previous(relaxed_coarse), force_fine)
    residual = fine_decay[None] * to_eigen(reaction(second_fine) + force_coarse) - to_eigen(relaxed_coarse)

    def coarse_turn(carry, term):
        updated = coarse_decay * carry + term
        return (updated, updated)
    unused, correction = lax.scan(coarse_turn, carried_correction, residual)
    coarse_states = relaxed_coarse + from_eigen(correction)
    fine_states = propagate(previous(coarse_states), force_fine)
    return (fine_states, coarse_states)
```

```python
import jax
import jax.numpy as jnp
from jax import lax
from jax.experimental import pallas as pl
from jax.experimental.pallas import tpu as pltpu
from jax.sharding import PartitionSpec as P

MESH = pl.DeviceIdType.MESH
F32 = jnp.float32
BF16 = jnp.bfloat16
TM = 16
SPACE = 8
N = 1024
B = 128
H = B // 2
ORDER_OUT = (2, 1, 3, 0)
ORDER_IN = (0, 1, 3, 2)


def dot(a, b):
    return jnp.dot(a, b, preferred_element_type=F32)


def react(field):
    return field + 0.5 * jnp.tanh(field)


def split(x):
    hi = x.astype(BF16)
    return hi, (x - hi.astype(F32)).astype(BF16)


def kernel(
    init_h, guess_h, ff_h, fc_h, u_h, rates, carried_h,
    fs_o, cs_o,
    ubuf, uh, ul, th, tl, init, guess, ff, fc, carried,
    ga, ffn, nrf, nrfn, coef, coefp, csb,
    sw, w, sz, z_in, xs, yb, fd, rsum, yref, lacc, facc, srecv, ssend, crecv,
    u_sem, loc_sem, sh_send, sh_recv,
    w_send, w_recv, wb_send, wb_recv, z_send, z_recv,
    s_send, s_recv, c_send, c_recv, out_sem,
):
    tm = lax.axis_index("tm")
    me = lax.axis_index("space")
    zc = me // 2
    core = me % 2
    other = zc * 2 + (1 - core)
    nxt = lax.rem(tm + 1, TM)
    prv = lax.rem(tm + TM - 1, TM)

    def remote(src, dst, ss, rs, dev):
        return pltpu.make_async_remote_copy(
            src_ref=src, dst_ref=dst, send_sem=ss, recv_sem=rs, device_id=dev, device_id_type=MESH
        )

    u_copies = [
        pltpu.make_async_copy(u_h.at[pl.ds(i * 256, 256)], ubuf.at[pl.ds(i * 256, 256)], u_sem.at[i])
        for i in range(4)
    ]
    loads = [
        pltpu.make_async_copy(init_h, init, loc_sem.at[0]),
        pltpu.make_async_copy(guess_h, guess, loc_sem.at[1]),
        pltpu.make_async_copy(ff_h, ff, loc_sem.at[2]),
        pltpu.make_async_copy(fc_h, fc, loc_sem.at[3]),
        pltpu.make_async_copy(
            carried_h.at[pl.ds(pl.multiple_of(tm * 64, 64), 64), pl.ds(pl.multiple_of(me * B, B), B)],
            carried, loc_sem.at[4]),
    ]
    for c in u_copies:
        c.start()
    for c in loads:
        c.start()

    barrier = pltpu.get_barrier_semaphore()
    count = 0
    for d in range(1, SPACE):
        pl.semaphore_signal(barrier, inc=1, device_id=(tm, lax.rem(me + d, SPACE)), device_id_type=MESH)
        count += 1
    for d in range(1, TM):
        pl.semaphore_signal(barrier, inc=1, device_id=(lax.rem(tm + d, TM), me), device_id_type=MESH)
        count += 1
    for d in range(1, SPACE):
        for t in (nxt, prv):
            pl.semaphore_signal(barrier, inc=1, device_id=(t, lax.rem(me + d, SPACE)), device_id_type=MESH)
            count += 1
    pl.semaphore_wait(barrier, count)

    top, low = pl.ds(0, H), pl.ds(H, H)
    guess_shift = remote(guess_h.at[top], ga, sh_send.at[0], sh_recv.at[0], (nxt, me))
    force_shift = remote(ff_h.at[low], ffn.at[low], sh_send.at[1], sh_recv.at[1], (prv, me))
    guess_shift.start()
    force_shift.start()
    force_rest = remote(ff_h.at[top], ffn.at[top], sh_send.at[2], sh_recv.at[2], (prv, me))
    nrf_shift = remote(nrf, nrfn, sh_send.at[3], sh_recv.at[3], (prv, me))
    coef_shift = remote(coef, coefp, sh_send.at[4], sh_recv.at[4], (nxt, me))
    cs_shift = remote(csb, cs_o, sh_send.at[5], sh_recv.at[5], (prv, me))

    for i in range(4):
        u_copies[i].wait()

    def prep(i, carry):
        at = pl.ds(pl.multiple_of(i * B, B), B)
        hi, lo = split(ubuf[at, :])
        uh[at, :] = hi
        ul[at, :] = lo
        return carry

    lax.fori_loop(0, 8, prep, 0)

    own = rates[:, pl.ds(pl.multiple_of(me * B, B), B)]

    def prep_decay(i, carry):
        at = pl.ds(pl.multiple_of(i * B, B), B)
        down = jnp.broadcast_to(rates[:, at], (B, B)).T
        s = down + jnp.broadcast_to(own, (B, B))
        rsum[at, :] = s
        fd[at, :] = 1.0 / (1.0 + s)
        return carry

    lax.fori_loop(0, 8, prep_decay, 0)

    def prep_t(i, carry):
        at = pl.ds(pl.multiple_of(i * B, B), B)
        hi, lo = split(ubuf[at, :].T)
        th[:, at] = hi
        tl[:, at] = lo
        return carry

    def chip_of(q):
        return lax.rem(zc + q, 4)

    def right_send(first):
        xh = xs[pl.ds(0, B), :]
        for q in ORDER_OUT:
            zd = chip_of(q)
            cols = pl.ds(pl.multiple_of(zd * 256, 256), 256)
            a = dot(xs[...], uh[:, cols])
            p = a[:B] + a[B:] + dot(xh, ul[:, cols])
            sw[zd * 2] = p[:, :B]
            sw[zd * 2 + 1] = p[:, B:]
            for c in range(2):
                d = zd * 2 + c
                if first:
                    ca = remote(sw.at[d, top], w.at[me, top], w_send.at[d], w_recv.at[me], (tm, d))
                    cb = remote(sw.at[d, low], w.at[me, low], wb_send.at[d], wb_recv.at[me], (nxt, d))
                    cb.start()
                else:
                    ca = remote(sw.at[d], w.at[me], w_send.at[d], w_recv.at[me], (tm, d))
                if q:
                    ca.start()
                else:
                    pl.when(core != c)(ca.start)
        if first:
            w[me, top] = sw[me, top]
        else:
            w[me] = sw[me]

    def wait_w(s, first, full):
        if first:
            remote(sw.at[s, low], w.at[s, low], wb_send.at[s], wb_recv.at[s], (prv, s)).wait_recv()
        if full:
            if first:
                remote(sw.at[s, top], w.at[s, top], w_send.at[s], w_recv.at[s], (tm, s)).wait_recv()
            else:
                remote(sw.at[s], w.at[s], w_send.at[s], w_recv.at[s], (tm, s)).wait_recv()

    def wait_w_sent(d, first, full):
        if first:
            remote(sw.at[d, low], w.at[me, low], wb_send.at[d], wb_recv.at[me], (nxt, d)).wait_send()
        if full:
            if first:
                remote(sw.at[d, top], w.at[me, top], w_send.at[d], w_recv.at[me], (tm, d)).wait_send()
            else:
                remote(sw.at[d], w.at[me], w_send.at[d], w_recv.at[me], (tm, d)).wait_send()

    for c in loads:
        c.wait()
    guess_shift.wait_recv()
    x = react(jnp.where(tm == 0, init[top, :], ga[...])) + ff[top, :]
    hi, lo = split(x)
    xs[pl.ds(0, H), :] = hi
    xs[pl.ds(B, H), :] = lo
    force_shift.wait_recv()
    x = react(jnp.where(tm == TM - 1, init[low, :], guess[low, :])) + ffn[low, :]
    hi, lo = split(x)
    xs[pl.ds(H, H), :] = hi
    xs[pl.ds(B + H, H), :] = lo
    right_send(True)
    force_rest.start()
    lax.fori_loop(0, 8, prep_t, 0)

    def scan_groups():
        for d in range(1, TM):
            e = lax.rem(tm + d, TM)
            remote(yref.at[e], srecv.at[tm], s_send.at[e], s_recv.at[tm], (e, me)).start()
        srecv[tm] = yref[tm]
        cd = 1.0 / (1.0 + 2.0 * rsum[pl.ds(pl.multiple_of(tm * 64, 64), 64), :])
        corr = carried[...]
        for d in range(1, TM):
            e = lax.rem(tm + d, TM)
            remote(yref.at[e], srecv.at[e], s_send.at[e], s_recv.at[e], (e, me)).wait_recv()
        for g in range(TM):
            corr = cd * corr + srecv[(g + TM - 1) % TM]
            ssend[g] = corr
            dest = (g + 1) % TM
            pl.when(tm != dest)(
                remote(ssend.at[g], crecv.at[tm], c_send.at[g], c_recv.at[tm], (dest, me)).start
            )
        crecv[tm] = ssend[prv]
        for d in range(1, TM):
            e = lax.rem(tm + d, TM)
            remote(ssend.at[e], crecv.at[e], c_send.at[e], c_recv.at[e], (e, me)).wait_recv()
        for d in range(1, TM):
            e = lax.rem(tm + d, TM)
            remote(yref.at[e], srecv.at[e], s_send.at[e], s_recv.at[e], (e, me)).wait_send()
        for g in range(TM):
            dest = (g + 1) % TM
            pl.when(tm != dest)(
                remote(ssend.at[g], crecv.at[tm], c_send.at[g], c_recv.at[tm], (dest, me)).wait_send
            )
        coef_shift.wait()
        yref[...] = coefp[...].reshape(TM, 64, B) + crecv[...]

    def turn(k, carry):
        for n, q in enumerate(ORDER_IN):
            zs = chip_of(q)

            def waits(first):
                if q:
                    wait_w(zs * 2, first, True)
                    wait_w(zs * 2 + 1, first, True)
                else:
                    wait_w(other, first, True)
                    if first:
                        wait_w(me, True, False)

            pl.when(k == 0)(lambda: waits(True))
            pl.when(k > 0)(lambda: waits(False))
            cols = pl.ds(pl.multiple_of(zs * 256, 256), 256)
            hi, lo = split(w[pl.ds(zs * 2, 2)].reshape(256, B))
            a = dot(th[:, cols], jnp.concatenate([hi, lo], axis=1))
            v = a[:, :B] + a[:, B:] + dot(tl[:, cols], hi)
            if n == 0:
                lacc[...] = v
            else:
                lacc[...] += v

        def sent(first):
            for q in (1, 2, 3):
                wait_w_sent(chip_of(q) * 2, first, True)
                wait_w_sent(chip_of(q) * 2 + 1, first, True)
            wait_w_sent(other, first, True)
            if first:
                wait_w_sent(me, True, False)

        pl.when(k == 0)(lambda: sent(True))
        pl.when(k > 0)(lambda: sent(False))

        yref[...] = (fd[...] * lacc[...]).reshape(TM, 64, B)

        @pl.when(k == 1)
        def _():
            coef[...] = yref[...].reshape(N, B)
            coef_shift.start()

        pl.when(k == 3)(scan_groups)

        hi, lo = split(yref[...].reshape(N, B))
        yb[:, pl.ds(0, B)] = hi
        yb[:, pl.ds(B, B)] = lo

        for q in ORDER_OUT:
            zd = chip_of(q)
            rows = pl.ds(pl.multiple_of(zd * 256, 256), 256)
            a = dot(uh[rows, :], yb[...])
            v = a[:, :B] + a[:, B:] + dot(ul[rows, :], yb[:, pl.ds(0, B)])
            sz[zd * 2] = v[:B]
            sz[zd * 2 + 1] = v[B:]
            for c in range(2):
                d = zd * 2 + c
                cp = remote(sz.at[d], z_in.at[me], z_send.at[d], z_recv.at[me], (tm, d))
                if q:
                    cp.start()
                else:
                    pl.when(core != c)(cp.start)
        z_in[me] = sz[me]

        for n, q in enumerate(ORDER_IN):
            zs = chip_of(q)
            sources = (zs * 2, zs * 2 + 1) if q else (other,)
            for s in sources:
                remote(sz.at[s], z_in.at[s], z_send.at[s], z_recv.at[s], (tm, s)).wait_recv()
            rows = pl.ds(pl.multiple_of(zs * 256, 256), 256)
            hi, lo = split(jnp.concatenate([z_in[zs * 2], z_in[zs * 2 + 1]], axis=1))
            a = dot(jnp.concatenate([hi, lo], axis=0), th[rows, :])
            v = a[:B] + a[B:] + dot(hi, tl[rows, :])
            if n == 0:
                facc[...] = v
            else:
                facc[...] += v
        for q in (1, 2, 3):
            for c in range(2):
                d = chip_of(q) * 2 + c
                remote(sz.at[d], z_in.at[me], z_send.at[d], z_recv.at[me], (tm, d)).wait_send()
        remote(sz.at[other], z_in.at[me], z_send.at[other], z_recv.at[me], (tm, other)).wait_send()

        @pl.when(k == 3)
        def _():
            csb[...] = facc[...]
            cs_shift.start()

        @pl.when(k < 4)
        def _():
            restart = ((k == 1) & (tm == TM - 1)) | ((k == 3) & (tm == 0))
            facc[...] = react(jnp.where(restart, init[...], facc[...]))

            @pl.when(k == 0)
            def _():
                nrf[...] = facc[...]
                nrf_shift.start()
                facc[...] += fc[...]

            @pl.when(k == 1)
            def _():
                force_shift.wait_send()
                force_rest.wait()
                facc[...] += ffn[...]

            @pl.when(k == 2)
            def _():
                nrf_shift.wait()
                facc[...] -= nrfn[...]

            @pl.when(k == 3)
            def _():
                facc[...] += ff[...]

            hi, lo = split(facc[...])
            xs[pl.ds(0, B), :] = hi
            xs[pl.ds(B, B), :] = lo
            right_send(False)

        return carry

    lax.fori_loop(0, 5, turn, 0)
    out = pltpu.make_async_copy(facc, fs_o, out_sem)
    out.start()
    guess_shift.wait_send()
    cs_shift.wait()
    out.wait()


def on_device(initial_state, guess_coarse, force_fine, force_coarse, eigen_basis, eigen_rates, carried_correction):
    vm, dma = pltpu.VMEM, pltpu.SemaphoreType.DMA
    any_spec = pl.BlockSpec(memory_space=pl.ANY)
    field = vm((B, N), F32)
    half = vm((H, N), F32)
    column = vm((N, B), F32)
    blocks = vm((SPACE, B, B), F32)
    parts = vm((TM, 64, B), F32)
    basis = vm((N, N), BF16)
    fine, coarse = pl.pallas_call(
        kernel,
        out_shape=(jax.ShapeDtypeStruct((B, N), F32), jax.ShapeDtypeStruct((B, N), F32)),
        in_specs=[any_spec] * 5 + [pl.BlockSpec(memory_space=pltpu.VMEM), any_spec],
        out_specs=(any_spec, any_spec),
        scratch_shapes=[
            vm((N, N), F32), basis, basis, basis, basis,
            field, field, field, field, vm((64, B), F32),
            half, field, field, field, column, column, field,
            blocks, blocks, blocks, blocks,
            vm((2 * B, N), BF16), vm((N, 2 * B), BF16),
            column, column, parts, column, field, parts, parts, parts,
            dma((4,)), dma((5,)), dma((6,)), dma((6,)),
            dma((8,)), dma((8,)), dma((8,)), dma((8,)), dma((8,)), dma((8,)),
            dma((16,)), dma((16,)), dma((16,)), dma((16,)), dma,
        ],
        compiler_params=pltpu.CompilerParams(
            collective_id=0, has_side_effects=True, vmem_limit_bytes=48 * 1024 * 1024
        ),
        name="mgrit_cycle",
    )(
        initial_state, guess_coarse[0], force_fine[0], force_coarse[0],
        eigen_basis, eigen_rates[None, :], carried_correction,
    )
    return fine[None], coarse[None]


def solution(mesh):
    rows = P("tm", "space", None)
    return jax.shard_map(
        on_device,
        mesh=mesh,
        in_specs=(P("space", None), rows, rows, rows, P(), P(), P()),
        out_specs=(rows, rows),
        check_vma=False,
    )
```

```python
import jax
import jax.numpy as jnp
from jax import lax
from jax.experimental import pallas as pl
from jax.experimental.pallas import tpu as pltpu
from jax.sharding import PartitionSpec as P

MESH = pl.DeviceIdType.MESH
F32 = jnp.float32
BF16 = jnp.bfloat16
TM = 16
SPACE = 8
N = 1024
B = 128
H = B // 2
Q = H // 2
M = N // 2
E = M // TM
ORDER_OUT = (2, 1, 3, 0)
ORDER_IN = (0, 1, 3, 2)


def dot(a, b):
    return jnp.dot(a, b, preferred_element_type=F32)


def react(field):
    return field + 0.5 * jnp.tanh(field)


def split(x):
    hi = x.astype(BF16)
    return hi, (x - hi.astype(F32)).astype(BF16)


def kernel(
    init_h, guess_h, ff_h, fc_h, u_h, rates, carried_h,
    fs_o, cs_o,
    ubuf, uh, ul, th, tl, lu, lt, init, guess, ff, fc, carried,
    ga, ffn, nrf, nrfn, coef, coefp, csb,
    sw, w, sz, z_in, xs, yb, fd, rsum, yref, lacc, facc, srecv, ssend, crecv,
    u_sem, loc_sem, ga_send, ga_recv, fb_send, fb_recv, fa_send, fa_recv,
    nr_send, nr_recv, co_send, co_recv, cs_send, cs_recv,
    w_send, w_recv, wb_send, wb_recv, z_send, z_recv,
    s_send, s_recv, c_send, c_recv,
):
    tm = lax.axis_index("tm")
    me = lax.axis_index("space")
    zc = me // 2
    core = me % 2
    other = zc * 2 + (1 - core)
    nxt = lax.rem(tm + 1, TM)
    prv = lax.rem(tm + TM - 1, TM)

    def remote(src, dst, ss, rs, dev):
        return pltpu.make_async_remote_copy(
            src_ref=src, dst_ref=dst, send_sem=ss, recv_sem=rs, device_id=dev, device_id_type=MESH
        )

    def chip_of(q):
        return lax.rem(zc + q, 4)

    u_copies = [
        pltpu.make_async_copy(u_h.at[pl.ds(i * 256, 256)], ubuf.at[pl.ds(i * 256, 256)], u_sem.at[i])
        for i in range(4)
    ]
    own_cols = pl.ds(pl.multiple_of(me * B, B), B)
    loads = [
        pltpu.make_async_copy(init_h, init, loc_sem.at[0]),
        pltpu.make_async_copy(guess_h, guess, loc_sem.at[1]),
        pltpu.make_async_copy(ff_h, ff, loc_sem.at[2]),
        pltpu.make_async_copy(fc_h, fc, loc_sem.at[3]),
    ] + [
        pltpu.make_async_copy(
            carried_h.at[pl.ds(pl.multiple_of(m * M + tm * E, E), E), own_cols], carried.at[m], loc_sem.at[4 + m])
        for m in range(2)
    ]
    for c in u_copies + loads:
        c.start()

    barrier = pltpu.get_barrier_semaphore()
    count = 0
    for d in range(1, SPACE):
        for t in (tm, nxt, prv):
            pl.semaphore_signal(barrier, inc=1, device_id=(t, lax.rem(me + d, SPACE)), device_id_type=MESH)
            count += 1
    for d in range(1, TM):
        pl.semaphore_signal(barrier, inc=1, device_id=(lax.rem(tm + d, TM), me), device_id_type=MESH)
        count += 1

    for c in u_copies:
        c.wait()

    def prep_natural(i, carry):
        at = pl.ds(pl.multiple_of(i * B, B), B)
        hi, lo = split(ubuf[at, :])
        uh[at, :] = hi
        ul[at, :] = lo
        hi, lo = split(ubuf[at, :].T)
        th[:, at] = hi
        tl[:, at] = lo
        return carry

    def prep_halves(j, carry):
        row = (j % 4) * 256 + (j // 4) * H
        x = jnp.concatenate(
            [ubuf[pl.ds(pl.multiple_of(row, H), H), :], ubuf[pl.ds(pl.multiple_of(row + B, H), H), :]], axis=0
        )
        hi, lo = split(x)
        lu[j, pl.ds(0, B), :] = hi
        lu[j, pl.ds(B, B), :] = lo
        at = pl.ds(pl.multiple_of(j * B, B), B)
        hi, lo = split(x.T)
        for m in range(2):
            lt[m, pl.ds(0, M), at] = hi[m * M:(m + 1) * M]
            lt[m, pl.ds(M, M), at] = lo[m * M:(m + 1) * M]
        return carry

    lax.fori_loop(0, 8, prep_natural, 0)
    own = rates[:, own_cols]

    def prep_decay(i, carry):
        at = pl.ds(pl.multiple_of(i * B, B), B)
        down = jnp.broadcast_to(rates[:, at], (B, B)).T
        s = down + jnp.broadcast_to(own, (B, B))
        rsum[at, :] = s
        fd[at, :] = 1.0 / (1.0 + s)
        return carry

    lax.fori_loop(0, 8, prep_decay, 0)
    for c in loads:
        c.wait()

    pl.semaphore_wait(barrier, count)

    def part_a(h):
        return pl.ds(h * H, Q)

    def part_b(h):
        return pl.ds(h * H + Q, Q)

    def rows_of(h):
        return pl.ds(h * H, H)

    guess_shift = [remote(guess_h.at[part_a(h)], ga.at[h], ga_send.at[h], ga_recv.at[h], (nxt, me)) for h in range(2)]
    force_b = [remote(ff_h.at[part_b(h)], ffn.at[part_b(h)], fb_send.at[h], fb_recv.at[h], (prv, me)) for h in range(2)]
    force_a = [remote(ff_h.at[part_a(h)], ffn.at[part_a(h)], fa_send.at[h], fa_recv.at[h], (prv, me)) for h in range(2)]
    nrf_shift = [remote(nrf.at[rows_of(h)], nrfn.at[rows_of(h)], nr_send.at[h], nr_recv.at[h], (prv, me)) for h in range(2)]
    coef_shift = remote(coef, coefp, co_send, co_recv, (nxt, me))
    cs_shift = [remote(csb.at[rows_of(h)], cs_o.at[rows_of(h)], cs_send.at[h], cs_recv.at[h], (prv, me)) for h in range(2)]
    for h in range(2):
        guess_shift[h].start()
        force_b[h].start()

    keep, give = pl.ds(0, Q), pl.ds(Q, Q)

    def w_copies(h, s, d, first):
        if not first:
            return (remote(sw.at[h, d], w.at[h, s], w_send.at[h, d], w_recv.at[h, s], (tm, d)),)
        return (
            remote(sw.at[h, d, keep], w.at[h, s, keep], w_send.at[h, d], w_recv.at[h, s], (tm, d)),
            remote(sw.at[h, d, give], w.at[h, s, give], wb_send.at[h, d], wb_recv.at[h, s], (nxt, d)),
        )

    def z_copy(h, s, d):
        return remote(sz.at[h, d], z_in.at[h, s], z_send.at[h, d], z_recv.at[h, s], (tm, d))

    def right_send(h, first):
        for q in ORDER_OUT:
            zd = chip_of(q)
            cols = pl.ds(pl.multiple_of(zd * 256, 256), 256)
            a = dot(xs[h], uh[:, cols])
            p = a[:H] + a[H:] + dot(xs[h, pl.ds(0, H), :], ul[:, cols])
            for c in range(2):
                d = zd * 2 + c
                sw[h, d] = p[:, c * B:(c + 1) * B]
                copies = w_copies(h, me, d, first)
                if q:
                    copies[0].start()
                else:
                    pl.when(core != c)(copies[0].start)
                if first:
                    copies[1].start()
        if first:
            w[h, me, keep] = sw[h, me, keep]
        else:
            w[h, me] = sw[h, me]

    def wait_w(h, q, first):
        if q:
            zs = chip_of(q)
            for s in (zs * 2, zs * 2 + 1):
                for c in w_copies(h, s, s, first):
                    c.wait_recv()
        else:
            for c in w_copies(h, other, other, first):
                c.wait_recv()
            if first:
                w_copies(h, me, me, True)[1].wait_recv()

    def wait_w_sent(first):
        for h in range(2):
            for q in (1, 2, 3):
                for i in range(2):
                    for c in w_copies(h, me, chip_of(q) * 2 + i, first):
                        c.wait_send()
            for c in w_copies(h, me, other, first):
                c.wait_send()
            if first:
                w_copies(h, me, me, True)[1].wait_send()

    def put_xs(h, x):
        hi, lo = split(x)
        xs[h, pl.ds(0, H), :] = hi
        xs[h, pl.ds(H, H), :] = lo

    for h in range(2):
        guess_shift[h].wait_recv()
        xa = react(jnp.where(tm == 0, init[part_a(h), :], ga[h])) + ff[part_a(h), :]
        force_b[h].wait_recv()
        xb = react(jnp.where(tm == TM - 1, init[part_b(h), :], guess[part_b(h), :])) + ffn[part_b(h), :]
        put_xs(h, jnp.concatenate([xa, xb], axis=0))
        right_send(h, True)
    for h in range(2):
        force_a[h].start()
    lax.fori_loop(0, 8, prep_halves, 0)

    def parts(m, e):
        return pl.ds(m * M + e * E, E)

    def s_copy(m, e, slot):
        at = pl.ds(pl.multiple_of(m * M + e * E, E), E)
        return remote(yref.at[at], srecv.at[m, slot], s_send.at[m, e], s_recv.at[m, slot], (e, me))

    def c_copy(m, g, dev, slot):
        return remote(ssend.at[m, g], crecv.at[m, slot], c_send.at[m, g], c_recv.at[m, slot], (dev, me))

    def send_residual(m):
        for d in range(1, TM):
            s_copy(m, lax.rem(tm + d, TM), tm).start()
        srecv[m, tm] = yref[pl.ds(pl.multiple_of(m * M + tm * E, E), E), :]

    def scan_groups():
        for m in range(2):
            cd = 1.0 / (1.0 + 2.0 * rsum[pl.ds(pl.multiple_of(m * M + tm * E, E), E), :])
            corr = carried[m]
            for d in range(1, TM):
                e = lax.rem(tm + d, TM)
                s_copy(m, e, e).wait_recv()
            for g in range(TM):
                corr = cd * corr + srecv[m, (g + TM - 1) % TM]
                ssend[m, g] = corr
                dest = (g + 1) % TM
                pl.when(tm != dest)(c_copy(m, g, dest, tm).start)
            crecv[m, tm] = ssend[m, prv]
        coef_shift.wait()
        for m in range(2):
            for d in range(1, TM):
                e = lax.rem(tm + d, TM)
                s_copy(m, e, tm).wait_send()
            for d in range(1, TM):
                e = lax.rem(tm + d, TM)
                c_copy(m, e, e, e).wait_recv()
            at = pl.ds(m * M, M)
            yref[at, :] = coefp[at, :] + crecv[m].reshape(M, B)
        for m in range(2):
            for g in range(TM):
                dest = (g + 1) % TM
                pl.when(tm != dest)(c_copy(m, g, dest, tm).wait_send)

    def turn(k, carry):
        def wide(x):
            hi, lo = split(x)
            return jnp.concatenate([hi, lo], axis=1)

        def left_part(m, cols, ww):
            a = dot(lt[m, :, cols], ww)
            return a[:M, :B] + a[:M, B:] + a[M:, :B]

        def waits(h, qs):
            def go(first):
                for q in qs:
                    wait_w(h, q, first)
            pl.when(k == 0)(lambda: go(True))
            pl.when(k > 0)(lambda: go(False))

        waits(0, ORDER_IN)
        ww = wide(w[0].reshape(M, B))
        for m in range(2):
            lacc[m] = left_part(m, pl.ds(0, M), ww)
        for n, q in enumerate(ORDER_IN):
            zs = chip_of(q)
            waits(1, (q,))
            cols = pl.ds(pl.multiple_of(M + zs * B, B), B)
            ww = wide(w[1, pl.ds(zs * 2, 2)].reshape(B, B))
            for m in range(2):
                v = lacc[m] + left_part(m, cols, ww)
                if n < 3:
                    lacc[m] = v
                else:
                    at = pl.ds(m * M, M)
                    yref[at, :] = fd[at, :] * v
                    pl.when(k == 3)(lambda m=m: send_residual(m))
        pl.when(k == 0)(lambda: wait_w_sent(True))
        pl.when(k > 0)(lambda: wait_w_sent(False))

        @pl.when(k == 1)
        def _():
            coef[...] = yref[...]
            coef_shift.start()

        pl.when(k == 3)(scan_groups)

        yb[...] = wide(yref[...])

        for h in range(2):
            for q in ORDER_OUT:
                zd = chip_of(q)
                a = dot(lu[h * 4 + zd], yb[...])
                v = a[:B, :B] + a[:B, B:] + a[B:, :B]
                for c in range(2):
                    d = zd * 2 + c
                    sz[h, d] = v[c * H:(c + 1) * H]
                    cp = z_copy(h, me, d)
                    if q:
                        cp.start()
                    else:
                        pl.when(core != c)(cp.start)
            z_in[h, me] = sz[h, me]

        for h in range(2):
            for q in ORDER_IN:
                zs = chip_of(q)
                for s in (zs * 2, zs * 2 + 1) if q else (other,):
                    z_copy(h, s, s).wait_recv()
            rows = rows_of(h)
            hi, lo = split(jnp.concatenate([z_in[h, s] for s in range(SPACE)], axis=1))
            a = dot(jnp.concatenate([hi, lo], axis=0), th[...])
            facc[rows, :] = a[:H] + a[H:] + dot(hi, tl[...])

            @pl.when(k == 3)
            def _():
                csb[rows, :] = facc[rows, :]
                cs_shift[h].start()

            @pl.when(k < 4)
            def _():
                restart = ((k == 1) & (tm == TM - 1)) | ((k == 3) & (tm == 0))
                facc[rows, :] = react(jnp.where(restart, init[rows, :], facc[rows, :]))

                @pl.when(k == 0)
                def _():
                    nrf[rows, :] = facc[rows, :]
                    nrf_shift[h].start()
                    facc[rows, :] += fc[rows, :]

                @pl.when(k == 1)
                def _():
                    force_b[h].wait_send()
                    force_a[h].wait()
                    facc[rows, :] += ffn[rows, :]

                @pl.when(k == 2)
                def _():
                    nrf_shift[h].wait()
                    facc[rows, :] -= nrfn[rows, :]

                @pl.when(k == 3)
                def _():
                    facc[rows, :] += ff[rows, :]

                put_xs(h, facc[rows, :])
                right_send(h, False)

        for h in range(2):
            for q in (1, 2, 3):
                for c in range(2):
                    z_copy(h, me, chip_of(q) * 2 + c).wait_send()
            z_copy(h, me, other).wait_send()
        return carry

    lax.fori_loop(0, 5, turn, 0)
    fs_o[...] = facc[...]
    for h in range(2):
        guess_shift[h].wait_send()
        cs_shift[h].wait()


def on_device(initial_state, guess_coarse, force_fine, force_coarse, eigen_basis, eigen_rates, carried_correction):
    vm, dma = pltpu.VMEM, pltpu.SemaphoreType.DMA
    hbm = pl.BlockSpec(memory_space=pl.ANY)
    vmem = pl.BlockSpec(memory_space=pltpu.VMEM)
    field = vm((B, N), F32)
    column = vm((N, B), F32)
    blocks = vm((2, SPACE, H, B), F32)
    shares = vm((2, TM, E, B), F32)
    basis = vm((N, N), BF16)
    two, eight, sixteen = dma((2,)), dma((2, SPACE)), dma((2, TM))
    fine, coarse = pl.pallas_call(
        kernel,
        out_shape=(jax.ShapeDtypeStruct((B, N), F32), jax.ShapeDtypeStruct((B, N), F32)),
        in_specs=[hbm] * 5 + [vmem, hbm],
        out_specs=(vmem, vmem),
        scratch_shapes=[
            vm((N, N), F32), basis, basis, basis, basis,
            vm((8, 2 * B, N), BF16), vm((2, N, N), BF16),
            field, field, field, field, vm((2, E, B), F32),
            vm((2, Q, N), F32), field, field, field, column, column, field,
            blocks, blocks, blocks, blocks,
            vm((2, B, N), BF16), vm((N, 2 * B), BF16),
            column, column, column, vm((2, M, B), F32), field, shares, shares, shares,
            dma((4,)), dma((6,)), two, two, two, two, two, two,
            two, two, dma, dma, two, two,
            eight, eight, eight, eight, eight, eight,
            sixteen, sixteen, sixteen, sixteen,
        ],
        compiler_params=pltpu.CompilerParams(
            collective_id=0, has_side_effects=True, vmem_limit_bytes=48 * 1024 * 1024
        ),
        name="mgrit_cycle",
    )(
        initial_state, guess_coarse[0], force_fine[0], force_coarse[0],
        eigen_basis, eigen_rates[None, :], carried_correction,
    )
    return fine[None], coarse[None]


def solution(mesh):
    rows = P("tm", "space", None)
    return jax.shard_map(
        on_device,
        mesh=mesh,
        in_specs=(P("space", None), rows, rows, rows, P(), P(), P()),
        out_specs=(rows, rows),
        check_vma=False,
    )
```

```python
import jax
import jax.numpy as jnp
from jax import lax
from jax.experimental import pallas as pl
from jax.experimental.pallas import tpu as pltpu
from jax.sharding import PartitionSpec as P

MESH = pl.DeviceIdType.MESH
F32 = jnp.float32
BF16 = jnp.bfloat16
TM = 16
SPACE = 8
N = 1024
B = 128
H = B // 2
Q = H // 2
M = N // 2
E = M // TM
FAR_FIRST = sorted(
    ((x, y) for x in range(4) for y in range(4) if x or y), key=lambda t: -min(t[0], 4 - t[0]) - min(t[1], 4 - t[1])
)


def dot(a, b):
    return jnp.dot(a, b, preferred_element_type=F32)


def react(field):
    return field + 0.5 * jnp.tanh(field)


def split(x):
    hi = x.astype(BF16)
    return hi, (x - hi.astype(F32)).astype(BF16)


def kernel(
    init_h, guess_h, ff_h, fc_h, u_h, rates, carried_h,
    fs_o, cs_o,
    ubuf, uh, ul, th, tl, lu, lt, init, guess, ff, fc, carried,
    ga, ffn, nrf, nrfn, coef, coefp, csb,
    sw, w, sz, z_in, xs, yb, fd, rsum, yref, lacc, facc, srecv, ssend, crecv,
    u_sem, loc_sem, ga_send, ga_recv, fb_send, fb_recv, fa_send, fa_recv,
    nr_send, nr_recv, co_send, co_recv, cs_send, cs_recv,
    w_send, w_recv, wb_send, wb_recv, z_send, z_recv,
    s_send, s_recv, c_send, c_recv,
):
    tm = lax.axis_index("tm")
    me = lax.axis_index("space")
    zc = me // 2
    core = me % 2
    other = zc * 2 + (1 - core)
    nxt = lax.rem(tm + 1, TM)
    prv = lax.rem(tm + TM - 1, TM)

    def remote(src, dst, ss, rs, dev):
        return pltpu.make_async_remote_copy(
            src_ref=src, dst_ref=dst, send_sem=ss, recv_sem=rs, device_id=dev, device_id_type=MESH
        )

    def chip_of(q):
        return lax.rem(zc + q, 4)

    def partner(chip):
        return chip + 1 - 2 * (chip % 2)

    far, near = chip_of(2), partner(zc)
    pairs = ((far // 2, (far, partner(far))), (zc // 2, (near, zc)))

    def group_at(dx, dy):
        return lax.rem(tm // 4 + dx, 4) * 4 + lax.rem(tm % 4 + dy, 4)

    u_copies = [
        pltpu.make_async_copy(u_h.at[pl.ds(i * 256, 256)], ubuf.at[pl.ds(i * 256, 256)], u_sem.at[i])
        for i in range(4)
    ]
    own_cols = pl.ds(pl.multiple_of(me * B, B), B)
    loads = [
        pltpu.make_async_copy(init_h, init, loc_sem.at[0]),
        pltpu.make_async_copy(guess_h, guess, loc_sem.at[1]),
        pltpu.make_async_copy(ff_h, ff, loc_sem.at[2]),
        pltpu.make_async_copy(fc_h, fc, loc_sem.at[3]),
    ] + [
        pltpu.make_async_copy(
            carried_h.at[pl.ds(pl.multiple_of(m * M + tm * E, E), E), own_cols], carried.at[m], loc_sem.at[4 + m])
        for m in range(2)
    ]
    for c in u_copies + loads:
        c.start()

    barrier = pltpu.get_barrier_semaphore()
    count = 0
    for d in range(1, SPACE):
        for t in (tm, nxt, prv):
            pl.semaphore_signal(barrier, inc=1, device_id=(t, lax.rem(me + d, SPACE)), device_id_type=MESH)
            count += 1
    for d in range(1, TM):
        pl.semaphore_signal(barrier, inc=1, device_id=(lax.rem(tm + d, TM), me), device_id_type=MESH)
        count += 1

    for c in loads:
        c.wait()
    pl.semaphore_wait(barrier, count)

    def part_a(h):
        return pl.ds(h * H, Q)

    def part_b(h):
        return pl.ds(h * H + Q, Q)

    def rows_of(h):
        return pl.ds(h * H, H)

    guess_shift = [remote(guess.at[part_a(h)], ga.at[h], ga_send.at[h], ga_recv.at[h], (nxt, me)) for h in range(2)]
    force_b = [remote(ff.at[part_b(h)], ffn.at[part_b(h)], fb_send.at[h], fb_recv.at[h], (prv, me)) for h in range(2)]
    force_a = [remote(ff.at[part_a(h)], ffn.at[part_a(h)], fa_send.at[h], fa_recv.at[h], (prv, me)) for h in range(2)]
    nrf_shift = [remote(nrf.at[rows_of(h)], nrfn.at[rows_of(h)], nr_send.at[h], nr_recv.at[h], (prv, me)) for h in range(2)]
    coef_shift = remote(coef, coefp, co_send, co_recv, (nxt, me))
    cs_shift = [remote(csb.at[rows_of(h)], cs_o.at[rows_of(h)], cs_send.at[h], cs_recv.at[h], (prv, me)) for h in range(2)]
    for h in range(2):
        guess_shift[h].start()
        force_b[h].start()

    for c in u_copies:
        c.wait()

    def prep_natural(i, carry):
        at = pl.ds(pl.multiple_of(i * B, B), B)
        hi, lo = split(ubuf[at, :])
        uh[at, :] = hi
        ul[at, :] = lo
        hi, lo = split(ubuf[at, :].T)
        th[:, at] = hi
        tl[:, at] = lo
        return carry

    def prep_halves(j, carry):
        row = (j % 4) * 256 + (j // 4) * H
        x = jnp.concatenate(
            [ubuf[pl.ds(pl.multiple_of(row, H), H), :], ubuf[pl.ds(pl.multiple_of(row + B, H), H), :]], axis=0
        )
        hi, lo = split(x)
        at = pl.multiple_of(j % 2 * B, B)
        lu[j // 2, pl.ds(at, B), :] = hi
        lu[j // 2, pl.ds(2 * B + at, B), :] = lo
        at = pl.ds(pl.multiple_of(j * B, B), B)
        hi, lo = split(x.T)
        for m in range(2):
            lt[m, pl.ds(0, M), at] = hi[m * M:(m + 1) * M]
            lt[m, pl.ds(M, M), at] = lo[m * M:(m + 1) * M]
        return carry

    lax.fori_loop(0, 8, prep_natural, 0)
    own = rates[:, own_cols]

    def prep_decay(i, carry):
        at = pl.ds(pl.multiple_of(i * B, B), B)
        down = jnp.broadcast_to(rates[:, at], (B, B)).T
        s = down + jnp.broadcast_to(own, (B, B))
        rsum[at, :] = s
        fd[at, :] = 1.0 / (1.0 + s)
        return carry

    lax.fori_loop(0, 8, prep_decay, 0)

    keep, give = pl.ds(0, Q), pl.ds(Q, Q)

    def w_copies(h, s, d, first):
        if not first:
            return (remote(sw.at[h, d], w.at[h, s], w_send.at[h, d], w_recv.at[h, s], (tm, d)),)
        return (
            remote(sw.at[h, d, keep], w.at[h, s, keep], w_send.at[h, d], w_recv.at[h, s], (tm, d)),
            remote(sw.at[h, d, give], w.at[h, s, give], wb_send.at[h, d], wb_recv.at[h, s], (nxt, d)),
        )

    def z_copy(h, s, d):
        return remote(sz.at[h, d], z_in.at[h, s], z_send.at[h, d], z_recv.at[h, s], (tm, d))

    def right_send(h, first):
        for pr, chips in pairs:
            cols = pl.ds(pl.multiple_of(pr * M, M), M)
            a = dot(xs[h], uh[:, cols])
            p = a[:H] + a[H:] + dot(xs[h, pl.ds(0, H), :], ul[:, cols])
            for i in range(4):
                sw[h, pr * 4 + i] = p[:, i * B:(i + 1) * B]
            for zd in chips:
                for c in range(2):
                    copies = w_copies(h, me, zd * 2 + c, first)
                    if zd is zc:
                        pl.when(core != c)(copies[0].start)
                    else:
                        copies[0].start()
                    if first:
                        copies[1].start()
        if first:
            w[h, me, keep] = sw[h, me, keep]
        else:
            w[h, me] = sw[h, me]

    def wait_w(h, q, first):
        if q:
            zs = chip_of(q)
            for s in (zs * 2, zs * 2 + 1):
                for c in w_copies(h, s, s, first):
                    c.wait_recv()
        else:
            for c in w_copies(h, other, other, first):
                c.wait_recv()
            if first:
                w_copies(h, me, me, True)[1].wait_recv()

    def wait_w_sent(first):
        for h in range(2):
            for q in (1, 2, 3):
                for i in range(2):
                    for c in w_copies(h, me, chip_of(q) * 2 + i, first):
                        c.wait_send()
            for c in w_copies(h, me, other, first):
                c.wait_send()
            if first:
                w_copies(h, me, me, True)[1].wait_send()

    def put_xs(h, x):
        hi, lo = split(x)
        xs[h, pl.ds(0, H), :] = hi
        xs[h, pl.ds(H, H), :] = lo

    for h in range(2):
        guess_shift[h].wait_recv()
        xa = react(jnp.where(tm == 0, init[part_a(h), :], ga[h])) + ff[part_a(h), :]
        force_b[h].wait_recv()
        xb = react(jnp.where(tm == TM - 1, init[part_b(h), :], guess[part_b(h), :])) + ffn[part_b(h), :]
        put_xs(h, jnp.concatenate([xa, xb], axis=0))
        right_send(h, True)
    for h in range(2):
        force_a[h].start()
    lax.fori_loop(0, 8, prep_halves, 0)

    def parts(m, e):
        return pl.ds(m * M + e * E, E)

    def s_copy(m, e, slot):
        at = pl.ds(pl.multiple_of(m * M + e * E, E), E)
        return remote(yref.at[at], srecv.at[m, slot], s_send.at[m, e], s_recv.at[m, slot], (e, me))

    def c_copy(m, g, dev, slot):
        return remote(ssend.at[m, g], crecv.at[m, slot], c_send.at[m, g], c_recv.at[m, slot], (dev, me))

    def send_residual(m):
        for dx, dy in FAR_FIRST:
            s_copy(m, group_at(dx, dy), tm).start()
        srecv[m, tm] = yref[pl.ds(pl.multiple_of(m * M + tm * E, E), E), :]

    def scan_groups():
        for m in range(2):
            cd = 1.0 / (1.0 + 2.0 * rsum[pl.ds(pl.multiple_of(m * M + tm * E, E), E), :])
            corr = carried[m]
            for d in range(1, TM):
                e = lax.rem(tm + d, TM)
                s_copy(m, e, e).wait_recv()
            for g in range(TM):
                corr = cd * corr + srecv[m, (g + TM - 1) % TM]
                ssend[m, (g + 1) % TM] = corr
            for dx, dy in FAR_FIRST:
                dest = group_at(dx, dy)
                c_copy(m, dest, dest, tm).start()
            crecv[m, tm] = ssend[m, tm]
        coef_shift.wait()
        for m in range(2):
            for d in range(1, TM):
                e = lax.rem(tm + d, TM)
                s_copy(m, e, tm).wait_send()
            for d in range(1, TM):
                e = lax.rem(tm + d, TM)
                c_copy(m, e, e, e).wait_recv()
            at = pl.ds(m * M, M)
            yref[at, :] = coefp[at, :] + crecv[m].reshape(M, B)
        for m in range(2):
            for d in range(1, TM):
                e = lax.rem(tm + d, TM)
                c_copy(m, e, e, tm).wait_send()

    def turn(k, carry):
        def wide(x):
            hi, lo = split(x)
            return jnp.concatenate([hi, lo], axis=1)

        def left_part(m, cols, ww):
            a = dot(lt[m, :, cols], ww)
            return a[:M, :B] + a[:M, B:] + a[M:, :B]

        def waits(h, qs):
            def go(first):
                for q in qs:
                    wait_w(h, q, first)
            pl.when(k == 0)(lambda: go(True))
            pl.when(k > 0)(lambda: go(False))

        waits(0, range(4))
        ww = wide(w[0].reshape(M, B))
        for m in range(2):
            lacc[m] = left_part(m, pl.ds(0, M), ww)
        waits(1, range(4))
        ww = wide(w[1].reshape(M, B))
        for m in range(2):
            at = pl.ds(m * M, M)
            yref[at, :] = fd[at, :] * (lacc[m] + left_part(m, pl.ds(M, M), ww))
            pl.when(k == 3)(lambda m=m: send_residual(m))
        pl.when(k == 0)(lambda: wait_w_sent(True))
        pl.when(k > 0)(lambda: wait_w_sent(False))

        @pl.when(k == 1)
        def _():
            coef[...] = yref[...]
            coef_shift.start()

        pl.when(k == 3)(scan_groups)

        yb[...] = wide(yref[...])

        for h in range(2):
            for pr, chips in pairs:
                a = dot(lu[h * 2 + pr], yb[...])
                v = a[:2 * B, :B] + a[:2 * B, B:] + a[2 * B:, :B]
                for i in range(4):
                    sz[h, pr * 4 + i] = v[i * H:(i + 1) * H]
                for zd in chips:
                    for c in range(2):
                        cp = z_copy(h, me, zd * 2 + c)
                        if zd is zc:
                            pl.when(core != c)(cp.start)
                        else:
                            cp.start()
            z_in[h, me] = sz[h, me]

        for h in range(2):
            for q in range(4):
                zs = chip_of(q)
                for s in (zs * 2, zs * 2 + 1) if q else (other,):
                    z_copy(h, s, s).wait_recv()
            rows = rows_of(h)
            hi, lo = split(jnp.concatenate([z_in[h, s] for s in range(SPACE)], axis=1))
            a = dot(jnp.concatenate([hi, lo], axis=0), th[...])
            facc[rows, :] = a[:H] + a[H:] + dot(hi, tl[...])

            @pl.when(k == 3)
            def _():
                csb[rows, :] = facc[rows, :]
                cs_shift[h].start()

            @pl.when(k < 4)
            def _():
                restart = ((k == 1) & (tm == TM - 1)) | ((k == 3) & (tm == 0))
                facc[rows, :] = react(jnp.where(restart, init[rows, :], facc[rows, :]))

                @pl.when(k == 0)
                def _():
                    nrf[rows, :] = facc[rows, :]
                    nrf_shift[h].start()
                    facc[rows, :] += fc[rows, :]

                @pl.when(k == 1)
                def _():
                    force_b[h].wait_send()
                    force_a[h].wait()
                    facc[rows, :] += ffn[rows, :]

                @pl.when(k == 2)
                def _():
                    nrf_shift[h].wait()
                    facc[rows, :] -= nrfn[rows, :]

                @pl.when(k == 3)
                def _():
                    facc[rows, :] += ff[rows, :]

                put_xs(h, facc[rows, :])
                right_send(h, False)

        for h in range(2):
            for q in (1, 2, 3):
                for c in range(2):
                    z_copy(h, me, chip_of(q) * 2 + c).wait_send()
            z_copy(h, me, other).wait_send()
        return carry

    lax.fori_loop(0, 5, turn, 0)
    fs_o[...] = facc[...]
    for h in range(2):
        guess_shift[h].wait_send()
        cs_shift[h].wait()


def on_device(initial_state, guess_coarse, force_fine, force_coarse, eigen_basis, eigen_rates, carried_correction):
    vm, dma = pltpu.VMEM, pltpu.SemaphoreType.DMA
    hbm = pl.BlockSpec(memory_space=pl.ANY)
    vmem = pl.BlockSpec(memory_space=pltpu.VMEM)
    field = vm((B, N), F32)
    column = vm((N, B), F32)
    blocks = vm((2, SPACE, H, B), F32)
    shares = vm((2, TM, E, B), F32)
    basis = vm((N, N), BF16)
    two, eight, sixteen = dma((2,)), dma((2, SPACE)), dma((2, TM))
    fine, coarse = pl.pallas_call(
        kernel,
        out_shape=(jax.ShapeDtypeStruct((B, N), F32), jax.ShapeDtypeStruct((B, N), F32)),
        in_specs=[hbm] * 5 + [vmem, hbm],
        out_specs=(vmem, vmem),
        scratch_shapes=[
            vm((N, N), F32), basis, basis, basis, basis,
            vm((4, 4 * B, N), BF16), vm((2, N, N), BF16),
            field, field, field, field, vm((2, E, B), F32),
            vm((2, Q, N), F32), field, field, field, column, column, field,
            blocks, blocks, blocks, blocks,
            vm((2, B, N), BF16), vm((N, 2 * B), BF16),
            column, column, column, vm((2, M, B), F32), field, shares, shares, shares,
            dma((4,)), dma((6,)), two, two, two, two, two, two,
            two, two, dma, dma, two, two,
            eight, eight, eight, eight, eight, eight,
            sixteen, sixteen, sixteen, sixteen,
        ],
        compiler_params=pltpu.CompilerParams(
            collective_id=0, has_side_effects=True, vmem_limit_bytes=56000000
        ),
        name="mgrit_cycle",
    )(
        initial_state, guess_coarse[0], force_fine[0], force_coarse[0],
        eigen_basis, eigen_rates[None, :], carried_correction,
    )
    return fine[None], coarse[None]


def solution(mesh):
    rows = P("tm", "space", None)
    return jax.shard_map(
        on_device,
        mesh=mesh,
        in_specs=(P("space", None), rows, rows, rows, P(), P(), P()),
        out_specs=(rows, rows),
        check_vma=False,
    )
```

```python
import jax
import jax.numpy as jnp
from jax import lax
from jax.experimental import pallas as pl
from jax.experimental.pallas import tpu as pltpu
from jax.sharding import PartitionSpec as P

MESH = pl.DeviceIdType.MESH
F32 = jnp.float32
BF16 = jnp.bfloat16
TM = 16
SPACE = 8
N = 1024
B = 128
H = B // 2
Q = H // 2
M = N // 2
E = B // TM
FAR_FIRST = sorted(
    ((x, y) for x in range(4) for y in range(4) if x or y), key=lambda t: -min(t[0], 4 - t[0]) - min(t[1], 4 - t[1])
)


def dot(a, b):
    return jnp.dot(a, b, preferred_element_type=F32)


def react(field):
    return field + 0.5 * jnp.tanh(field)


def split(x):
    hi = x.astype(BF16)
    return hi, (x - hi.astype(F32)).astype(BF16)


def kernel(
    init_h, guess_h, ff_h, fc_h, u_h, rates, carried_h,
    fs_o, cs_o,
    ubuf, uh, ul, th, tl, uph, upl, tph, tpl, init, guess, ff, fc, cbuf, carried,
    ga, ffn, nrf, nrfn, coef, coefp, csb,
    sw, w, sz, z_in, xs, yb, fd, rsum, yref, lacc, facc, srecv, ssend, crecv,
    u_sem, loc_sem, ga_send, ga_recv, fb_send, fb_recv, fa_send, fa_recv,
    nr_send, nr_recv, co_send, co_recv, cs_send, cs_recv,
    w_send, w_recv, wb_send, wb_recv, z_send, z_recv,
    s_send, s_recv, c_send, c_recv,
):
    tm = lax.axis_index("tm")
    me = lax.axis_index("space")
    zc = me // 2
    core = me % 2
    other = zc * 2 + (1 - core)
    nxt = lax.rem(tm + 1, TM)
    prv = lax.rem(tm + TM - 1, TM)

    def remote(src, dst, ss, rs, dev):
        return pltpu.make_async_remote_copy(
            src_ref=src, dst_ref=dst, send_sem=ss, recv_sem=rs, device_id=dev, device_id_type=MESH
        )

    def chip_of(q):
        return lax.rem(zc + q, 4)

    def partner(chip):
        return chip + 1 - 2 * (chip % 2)

    far, near = chip_of(2), partner(zc)
    pairs = ((far // 2, (far, partner(far))), (zc // 2, (near, zc)))

    def group_at(dx, dy):
        return lax.rem(tm // 4 + dx, 4) * 4 + lax.rem(tm % 4 + dy, 4)

    u_copies = [
        pltpu.make_async_copy(u_h.at[pl.ds(i * 256, 256)], ubuf.at[pl.ds(i * 256, 256)], u_sem.at[i])
        for i in range(4)
    ]
    own_cols = pl.ds(pl.multiple_of(me * B, B), B)
    loads = [
        pltpu.make_async_copy(init_h, init, loc_sem.at[0]),
        pltpu.make_async_copy(guess_h, guess, loc_sem.at[1]),
        pltpu.make_async_copy(ff_h, ff, loc_sem.at[2]),
        pltpu.make_async_copy(fc_h, fc, loc_sem.at[3]),
        pltpu.make_async_copy(carried_h.at[:, own_cols], cbuf, loc_sem.at[4]),
    ]
    for c in u_copies + loads:
        c.start()

    barrier = pltpu.get_barrier_semaphore()
    count = 0
    for d in range(1, SPACE):
        for t in (tm, nxt, prv):
            pl.semaphore_signal(barrier, inc=1, device_id=(t, lax.rem(me + d, SPACE)), device_id_type=MESH)
            count += 1
    for d in range(1, TM):
        pl.semaphore_signal(barrier, inc=1, device_id=(lax.rem(tm + d, TM), me), device_id_type=MESH)
        count += 1

    for c in loads:
        c.wait()
    pl.semaphore_wait(barrier, count)

    def part_a(h):
        return pl.ds(h * H, Q)

    def part_b(h):
        return pl.ds(h * H + Q, Q)

    def rows_of(h):
        return pl.ds(h * H, H)

    guess_shift = [remote(guess.at[part_a(h)], ga.at[h], ga_send.at[h], ga_recv.at[h], (nxt, me)) for h in range(2)]
    force_b = [remote(ff.at[part_b(h)], ffn.at[part_b(h)], fb_send.at[h], fb_recv.at[h], (prv, me)) for h in range(2)]
    force_a = [remote(ff.at[part_a(h)], ffn.at[part_a(h)], fa_send.at[h], fa_recv.at[h], (prv, me)) for h in range(2)]
    nrf_shift = [remote(nrf.at[rows_of(h)], nrfn.at[rows_of(h)], nr_send.at[h], nr_recv.at[h], (prv, me)) for h in range(2)]
    coef_shift = remote(coef, coefp, co_send, co_recv, (nxt, me))
    cs_shift = [remote(csb.at[rows_of(h)], cs_o.at[rows_of(h)], cs_send.at[h], cs_recv.at[h], (prv, me)) for h in range(2)]
    for h in range(2):
        guess_shift[h].start()
        force_b[h].start()

    for c in u_copies:
        c.wait()

    def prep_natural(i, carry):
        at = pl.ds(pl.multiple_of(i * B, B), B)
        hi, lo = split(ubuf[at, :])
        uh[at, :] = hi
        ul[at, :] = lo
        hi, lo = split(ubuf[at, :].T)
        th[:, at] = hi
        tl[:, at] = lo
        return carry

    def prep_halves(j, carry):
        row = (j % 4) * 256 + (j // 4) * H
        first, second = pl.ds(pl.multiple_of(row, H), H), pl.ds(pl.multiple_of(row + B, H), H)
        at = pl.ds(pl.multiple_of(j % 4 * B, B), B)
        x = jnp.concatenate([ubuf[first, :], ubuf[second, :]], axis=0)
        hi, lo = split(x)
        uph[j // 4, at, :] = hi
        upl[j // 4, at, :] = lo
        hi, lo = split(x.T)
        tph[j // 4, :, at] = hi
        tpl[j // 4, :, at] = lo
        return carry

    lax.fori_loop(0, 8, prep_natural, 0)
    own = rates[:, own_cols]

    own_down = jnp.broadcast_to(own, (B, B)).T

    def prep_decay(i, carry):
        at = pl.ds(pl.multiple_of(i * B, B), B)
        half = pl.ds(pl.multiple_of(i % 4 * B, B), B)
        total = jnp.broadcast_to(rates[:, at], (B, B)) + own_down
        rsum[i // 4, :, half] = total
        fd[i // 4, :, half] = 1.0 / (1.0 + total)
        carried[i // 4, :, half] = cbuf[at, :].T
        return carry

    lax.fori_loop(0, 8, prep_decay, 0)

    keep, give = pl.ds(0, Q), pl.ds(Q, Q)

    def w_copies(h, s, d, first):
        if not first:
            return (remote(sw.at[h, d], w.at[h, s], w_send.at[h, d], w_recv.at[h, s], (tm, d)),)
        return (
            remote(sw.at[h, d, keep], w.at[h, s, keep], w_send.at[h, d], w_recv.at[h, s], (tm, d)),
            remote(sw.at[h, d, give], w.at[h, s, give], wb_send.at[h, d], wb_recv.at[h, s], (nxt, d)),
        )

    def z_copy(h, s, d):
        return remote(sz.at[h, d], z_in.at[h, s], z_send.at[h, d], z_recv.at[h, s], (tm, d))

    def right_send(h, first):
        for pr, chips in pairs:
            cols = pl.ds(pl.multiple_of(pr * M, M), M)
            a = dot(xs[h], uh[:, cols])
            p = a[:H] + a[H:] + dot(xs[h, pl.ds(0, H), :], ul[:, cols])
            for i in range(4):
                sw[h, pr * 4 + i] = p[:, i * B:(i + 1) * B]
            for zd in chips:
                for c in range(2):
                    copies = w_copies(h, me, zd * 2 + c, first)
                    if zd is zc:
                        pl.when(core != c)(copies[0].start)
                    else:
                        copies[0].start()
                    if first:
                        copies[1].start()
        if first:
            w[h, me, keep] = sw[h, me, keep]
        else:
            w[h, me] = sw[h, me]

    def wait_w(h, q, first):
        if q:
            zs = chip_of(q)
            for s in (zs * 2, zs * 2 + 1):
                for c in w_copies(h, s, s, first):
                    c.wait_recv()
        else:
            for c in w_copies(h, other, other, first):
                c.wait_recv()
            if first:
                w_copies(h, me, me, True)[1].wait_recv()

    def wait_w_sent(first):
        for h in range(2):
            for q in (1, 2, 3):
                for i in range(2):
                    for c in w_copies(h, me, chip_of(q) * 2 + i, first):
                        c.wait_send()
            for c in w_copies(h, me, other, first):
                c.wait_send()
            if first:
                w_copies(h, me, me, True)[1].wait_send()

    def put_xs(h, x):
        hi, lo = split(x)
        xs[h, pl.ds(0, H), :] = hi
        xs[h, pl.ds(H, H), :] = lo

    for h in range(2):
        guess_shift[h].wait_recv()
        xa = react(jnp.where(tm == 0, init[part_a(h), :], ga[h])) + ff[part_a(h), :]
        force_b[h].wait_recv()
        xb = react(jnp.where(tm == TM - 1, init[part_b(h), :], guess[part_b(h), :])) + ffn[part_b(h), :]
        put_xs(h, jnp.concatenate([xa, xb], axis=0))
        right_send(h, True)
    for h in range(2):
        force_a[h].start()
    lax.fori_loop(0, 8, prep_halves, 0)

    def share(e):
        return pl.ds(pl.multiple_of(e * E, E), E)

    def s_copy(m, e, slot):
        return remote(yref.at[m, share(e)], srecv.at[m, slot], s_send.at[m, e], s_recv.at[m, slot], (e, me))

    def c_copy(m, g, dev, slot):
        return remote(ssend.at[m, g], crecv.at[m, slot], c_send.at[m, g], c_recv.at[m, slot], (dev, me))

    def send_residual(m):
        for dx, dy in FAR_FIRST:
            s_copy(m, group_at(dx, dy), tm).start()
        srecv[m, tm] = yref[m, share(tm), :]

    def scan_groups():
        for m in range(2):
            cd = 1.0 / (1.0 + 2.0 * rsum[m, share(tm), :])
            corr = carried[m, share(tm), :]
            for d in range(1, TM):
                e = lax.rem(tm + d, TM)
                s_copy(m, e, e).wait_recv()
            for g in range(TM):
                corr = cd * corr + srecv[m, (g + TM - 1) % TM]
                ssend[m, (g + 1) % TM] = corr
            for dx, dy in FAR_FIRST:
                dest = group_at(dx, dy)
                c_copy(m, dest, dest, tm).start()
            crecv[m, tm] = ssend[m, tm]
        coef_shift.wait()
        for m in range(2):
            for d in range(1, TM):
                e = lax.rem(tm + d, TM)
                s_copy(m, e, tm).wait_send()
            for d in range(1, TM):
                e = lax.rem(tm + d, TM)
                c_copy(m, e, e, e).wait_recv()
            yref[m] = coefp[m] + crecv[m].reshape(B, M)
        for m in range(2):
            for d in range(1, TM):
                e = lax.rem(tm + d, TM)
                c_copy(m, e, e, tm).wait_send()

    def turn(k, carry):
        def left_half(h):
            hi, lo = split(w[h].reshape(M, B).T)
            return hi, jnp.concatenate([hi, lo], axis=0)

        def left_part(h, m, hi, both):
            cols = pl.ds(m * M, M)
            a = dot(both, uph[h, :, cols])
            return a[:B] + a[B:] + dot(hi, upl[h, :, cols])

        def waits(h, qs):
            def go(first):
                for q in qs:
                    wait_w(h, q, first)
            pl.when(k == 0)(lambda: go(True))
            pl.when(k > 0)(lambda: go(False))

        waits(0, range(4))
        hi, both = left_half(0)
        for m in range(2):
            lacc[m] = left_part(0, m, hi, both)
        waits(1, range(4))
        hi, both = left_half(1)
        for m in range(2):
            yref[m] = fd[m] * (lacc[m] + left_part(1, m, hi, both))
            pl.when(k == 3)(lambda m=m: send_residual(m))
        pl.when(k == 0)(lambda: wait_w_sent(True))
        pl.when(k > 0)(lambda: wait_w_sent(False))

        @pl.when(k == 1)
        def _():
            coef[...] = yref[...]
            coef_shift.start()

        pl.when(k == 3)(scan_groups)

        for m in range(2):
            hi, lo = split(yref[m])
            yb[pl.ds(0, B), pl.ds(m * M, M)] = hi
            yb[pl.ds(B, B), pl.ds(m * M, M)] = lo

        for h in range(2):
            a = dot(yb[...], tph[h])
            v = a[:B] + a[B:] + dot(yb[pl.ds(0, B), :], tpl[h])
            sz[h] = v.T.reshape(SPACE, H, B)
            for zd in (far, partner(far), near, zc):
                for c in range(2):
                    cp = z_copy(h, me, zd * 2 + c)
                    if zd is zc:
                        pl.when(core != c)(cp.start)
                    else:
                        cp.start()
            z_in[h, me] = sz[h, me]

        for h in range(2):
            for q in range(4):
                zs = chip_of(q)
                for s in (zs * 2, zs * 2 + 1) if q else (other,):
                    z_copy(h, s, s).wait_recv()
            rows = rows_of(h)
            hi, lo = split(jnp.concatenate([z_in[h, s] for s in range(SPACE)], axis=1))
            a = dot(jnp.concatenate([hi, lo], axis=0), th[...])
            facc[rows, :] = a[:H] + a[H:] + dot(hi, tl[...])

            @pl.when(k == 3)
            def _():
                csb[rows, :] = facc[rows, :]
                cs_shift[h].start()

            @pl.when(k < 4)
            def _():
                restart = ((k == 1) & (tm == TM - 1)) | ((k == 3) & (tm == 0))
                facc[rows, :] = react(jnp.where(restart, init[rows, :], facc[rows, :]))

                @pl.when(k == 0)
                def _():
                    nrf[rows, :] = facc[rows, :]
                    nrf_shift[h].start()
                    facc[rows, :] += fc[rows, :]

                @pl.when(k == 1)
                def _():
                    force_b[h].wait_send()
                    force_a[h].wait()
                    facc[rows, :] += ffn[rows, :]

                @pl.when(k == 2)
                def _():
                    nrf_shift[h].wait()
                    facc[rows, :] -= nrfn[rows, :]

                @pl.when(k == 3)
                def _():
                    facc[rows, :] += ff[rows, :]

                put_xs(h, facc[rows, :])
                right_send(h, False)

        for h in range(2):
            for q in (1, 2, 3):
                for c in range(2):
                    z_copy(h, me, chip_of(q) * 2 + c).wait_send()
            z_copy(h, me, other).wait_send()
        return carry

    lax.fori_loop(0, 5, turn, 0)
    fs_o[...] = facc[...]
    for h in range(2):
        guess_shift[h].wait_send()
        cs_shift[h].wait()


def on_device(initial_state, guess_coarse, force_fine, force_coarse, eigen_basis, eigen_rates, carried_correction):
    vm, dma = pltpu.VMEM, pltpu.SemaphoreType.DMA
    hbm = pl.BlockSpec(memory_space=pl.ANY)
    vmem = pl.BlockSpec(memory_space=pltpu.VMEM)
    field = vm((B, N), F32)
    column = vm((N, B), F32)
    blocks = vm((2, SPACE, H, B), F32)
    pair = vm((2, B, M), F32)
    shares = vm((2, TM, E, M), F32)
    basis = vm((N, N), BF16)
    two, eight, sixteen = dma((2,)), dma((2, SPACE)), dma((2, TM))
    fine, coarse = pl.pallas_call(
        kernel,
        out_shape=(jax.ShapeDtypeStruct((B, N), F32), jax.ShapeDtypeStruct((B, N), F32)),
        in_specs=[hbm] * 5 + [vmem, hbm],
        out_specs=(vmem, vmem),
        scratch_shapes=[
            vm((N, N), F32), basis, basis, basis, basis,
            vm((2, M, N), BF16), vm((2, M, N), BF16), vm((2, N, M), BF16), vm((2, N, M), BF16),
            field, field, field, field, column, pair,
            vm((2, Q, N), F32), field, field, field, pair, pair, field,
            blocks, blocks, blocks, blocks,
            vm((2, B, N), BF16), vm((2 * B, N), BF16),
            pair, pair, pair, pair, field, shares, shares, shares,
            dma((4,)), dma((5,)), two, two, two, two, two, two,
            two, two, dma, dma, two, two,
            eight, eight, eight, eight, eight, eight,
            sixteen, sixteen, sixteen, sixteen,
        ],
        compiler_params=pltpu.CompilerParams(
            collective_id=0, has_side_effects=True, vmem_limit_bytes=55000000
        ),
        name="mgrit_cycle",
    )(
        initial_state, guess_coarse[0], force_fine[0], force_coarse[0],
        eigen_basis, eigen_rates[None, :], carried_correction,
    )
    return fine[None], coarse[None]


def solution(mesh):
    rows = P("tm", "space", None)
    return jax.shard_map(
        on_device,
        mesh=mesh,
        in_specs=(P("space", None), rows, rows, rows, P(), P(), P()),
        out_specs=(rows, rows),
        check_vma=False,
    )
```

```python
import jax
import jax.numpy as jnp
from jax import lax
from jax.experimental import pallas as pl
from jax.experimental.pallas import tpu as pltpu
from jax.sharding import PartitionSpec as P

MESH = pl.DeviceIdType.MESH
F32 = jnp.float32
BF16 = jnp.bfloat16
TM = 16
SPACE = 8
N = 1024
B = 128
H = B // 2
Q = H // 2
M = N // 2
E = B // TM
FAR_FIRST = sorted(
    ((x, y) for x in range(4) for y in range(4) if x or y), key=lambda t: -min(t[0], 4 - t[0]) - min(t[1], 4 - t[1])
)


def dot(a, b):
    return jnp.dot(a, b, preferred_element_type=F32)


def react(field):
    return field + 0.5 * jnp.tanh(field)


def split(x):
    hi = x.astype(BF16)
    return hi, (x - hi.astype(F32)).astype(BF16)


def kernel(
    init_h, guess_h, ff_h, fc_h, u_h, rates, carried_h,
    fs_o, cs_o,
    ubuf, uh, ul, th, tl, uph, upl, tph, tpl, init, guess, ff, fc, cbuf, carried,
    ga, ffn, nrf, nrfn, coef, coefp, csb,
    sw, w, sz, z_in, xs, yb, fd, rsum, yref, lacc, facc, srecv, ssend, crecv,
    u_sem, loc_sem, ga_send, ga_recv, fb_send, fb_recv, fa_send, fa_recv,
    nr_send, nr_recv, co_send, co_recv, cs_send, cs_recv,
    w_send, w_recv, wb_send, wb_recv, z_send, z_recv,
    s_send, s_recv, c_send, c_recv,
):
    tm = lax.axis_index("tm")
    me = lax.axis_index("space")
    zc = me // 2
    core = me % 2
    mine = core * 4 + zc
    nxt = lax.rem(tm + 1, TM)
    prv = lax.rem(tm + TM - 1, TM)

    def remote(src, dst, ss, rs, dev):
        return pltpu.make_async_remote_copy(
            src_ref=src, dst_ref=dst, send_sem=ss, recv_sem=rs, device_id=dev, device_id_type=MESH
        )

    def chip_of(q):
        return lax.rem(zc + q, 4)

    chips = (chip_of(2), chip_of(1), chip_of(3), zc)

    def group_at(dx, dy):
        return lax.rem(tm // 4 + dx, 4) * 4 + lax.rem(tm % 4 + dy, 4)

    u_copies = [
        pltpu.make_async_copy(u_h.at[pl.ds(i * 256, 256)], ubuf.at[pl.ds(i * 256, 256)], u_sem.at[i])
        for i in range(4)
    ]
    own_cols = pl.ds(pl.multiple_of(me * B, B), B)
    loads = [
        pltpu.make_async_copy(init_h, init, loc_sem.at[0]),
        pltpu.make_async_copy(guess_h, guess, loc_sem.at[1]),
        pltpu.make_async_copy(ff_h, ff, loc_sem.at[2]),
        pltpu.make_async_copy(fc_h, fc, loc_sem.at[3]),
        pltpu.make_async_copy(carried_h.at[:, own_cols], cbuf, loc_sem.at[4]),
    ]
    for c in u_copies + loads:
        c.start()

    barrier = pltpu.get_barrier_semaphore()
    count = 0
    for d in range(1, SPACE):
        for t in (tm, nxt, prv):
            pl.semaphore_signal(barrier, inc=1, device_id=(t, lax.rem(me + d, SPACE)), device_id_type=MESH)
            count += 1
    for d in range(1, TM):
        pl.semaphore_signal(barrier, inc=1, device_id=(lax.rem(tm + d, TM), me), device_id_type=MESH)
        count += 1

    for c in loads:
        c.wait()
    pl.semaphore_wait(barrier, count)

    def part_a(h):
        return pl.ds(h * H, Q)

    def part_b(h):
        return pl.ds(h * H + Q, Q)

    def rows_of(h):
        return pl.ds(h * H, H)

    guess_shift = [remote(guess.at[part_a(h)], ga.at[h], ga_send.at[h], ga_recv.at[h], (nxt, me)) for h in range(2)]
    force_b = [remote(ff.at[part_b(h)], ffn.at[part_b(h)], fb_send.at[h], fb_recv.at[h], (prv, me)) for h in range(2)]
    force_a = [remote(ff.at[part_a(h)], ffn.at[part_a(h)], fa_send.at[h], fa_recv.at[h], (prv, me)) for h in range(2)]
    nrf_shift = [remote(nrf.at[rows_of(h)], nrfn.at[rows_of(h)], nr_send.at[h], nr_recv.at[h], (prv, me)) for h in range(2)]
    coef_shift = remote(coef, coefp, co_send, co_recv, (nxt, me))
    cs_shift = [remote(csb.at[rows_of(h)], cs_o.at[rows_of(h)], cs_send.at[h], cs_recv.at[h], (prv, me)) for h in range(2)]
    for h in range(2):
        guess_shift[h].start()
        force_b[h].start()

    for c in u_copies:
        c.wait()

    def prep_natural(i, carry):
        at = pl.ds(pl.multiple_of(i * B, B), B)
        hi, lo = split(ubuf[at, :])
        for s in range(SPACE):
            old, new = slice(s * B, (s + 1) * B), pl.ds((s % 2 * 4 + s // 2) * B, B)
            uh[at, new] = hi[:, old]
            ul[at, new] = lo[:, old]
        hi, lo = split(ubuf[at, :].T)
        for s in range(SPACE):
            old, new = slice(s * B, (s + 1) * B), pl.ds((s % 2 * 4 + s // 2) * B, B)
            th[new, at] = hi[old]
            tl[new, at] = lo[old]
        return carry

    def prep_halves(j, carry):
        row = (j % 2 * 4 + j % 4 // 2) * B + (j // 4) * H
        first, second = pl.ds(pl.multiple_of(row, H), H), pl.ds(pl.multiple_of(row + 2 * B, H), H)
        at = pl.ds(pl.multiple_of(j % 4 * B, B), B)
        x = jnp.concatenate([ubuf[first, :], ubuf[second, :]], axis=0)
        hi, lo = split(x)
        uph[j // 4, at, :] = hi
        upl[j // 4, at, :] = lo
        hi, lo = split(x.T)
        tph[j // 4, :, at] = hi
        tpl[j // 4, :, at] = lo
        return carry

    lax.fori_loop(0, 8, prep_natural, 0)
    own = rates[:, own_cols]

    own_down = jnp.broadcast_to(own, (B, B)).T

    def prep_decay(i, carry):
        at = pl.ds(pl.multiple_of(i * B, B), B)
        half = pl.ds(pl.multiple_of(i % 4 * B, B), B)
        total = jnp.broadcast_to(rates[:, at], (B, B)) + own_down
        rsum[i // 4, :, half] = total
        fd[i // 4, :, half] = 1.0 / (1.0 + total)
        carried[i // 4, :, half] = cbuf[at, :].T
        return carry

    lax.fori_loop(0, 8, prep_decay, 0)

    keep, give = pl.ds(0, Q), pl.ds(Q, Q)

    def w_copies(h, s, chip, c, first):
        d, dev = c * 4 + chip, chip * 2 + c
        if not first:
            return (remote(sw.at[h, d], w.at[h, s], w_send.at[h, d], w_recv.at[h, s], (tm, dev)),)
        return (
            remote(sw.at[h, d, keep], w.at[h, s, keep], w_send.at[h, d], w_recv.at[h, s], (tm, dev)),
            remote(sw.at[h, d, give], w.at[h, s, give], wb_send.at[h, d], wb_recv.at[h, s], (nxt, dev)),
        )

    def z_copy(h, s, chip, c):
        d = c * 4 + chip
        return remote(sz.at[h, d], z_in.at[h, s], z_send.at[h, d], z_recv.at[h, s], (tm, chip * 2 + c))

    def unless_mine(chip, c, act):
        if chip is zc:
            pl.when(core != c)(act)
        else:
            act()

    def right_send(h, first):
        for c in range(2):
            cols = pl.ds(c * M, M)
            a = dot(xs[h], uh[:, cols])
            p = a[:H] + a[H:] + dot(xs[h, pl.ds(0, H), :], ul[:, cols])
            for i in range(4):
                sw[h, c * 4 + i] = p[:, i * B:(i + 1) * B]
            for chip in chips:
                copies = w_copies(h, mine, chip, c, first)
                unless_mine(chip, c, copies[0].start)
                if first:
                    copies[1].start()
        if first:
            w[h, mine, keep] = sw[h, mine, keep]
        else:
            w[h, mine] = sw[h, mine]

    def wait_w(h, c, first):
        for chip in chips:
            copies = w_copies(h, c * 4 + chip, chip, c, first)
            unless_mine(chip, c, copies[0].wait_recv)
            if first:
                copies[1].wait_recv()

    def wait_w_sent(first):
        for h in range(2):
            for c in range(2):
                for chip in chips:
                    copies = w_copies(h, mine, chip, c, first)
                    unless_mine(chip, c, copies[0].wait_send)
                    if first:
                        copies[1].wait_send()

    def put_xs(h, x):
        hi, lo = split(x)
        xs[h, pl.ds(0, H), :] = hi
        xs[h, pl.ds(H, H), :] = lo

    for h in range(2):
        guess_shift[h].wait_recv()
        xa = react(jnp.where(tm == 0, init[part_a(h), :], ga[h])) + ff[part_a(h), :]
        force_b[h].wait_recv()
        xb = react(jnp.where(tm == TM - 1, init[part_b(h), :], guess[part_b(h), :])) + ffn[part_b(h), :]
        put_xs(h, jnp.concatenate([xa, xb], axis=0))
        right_send(h, True)
    for h in range(2):
        force_a[h].start()
    lax.fori_loop(0, 8, prep_halves, 0)

    def share(e):
        return pl.ds(pl.multiple_of(e * E, E), E)

    def s_copy(m, e, slot):
        return remote(yref.at[m, share(e)], srecv.at[m, slot], s_send.at[m, e], s_recv.at[m, slot], (e, me))

    def c_copy(m, g, dev, slot):
        return remote(ssend.at[m, g], crecv.at[m, slot], c_send.at[m, g], c_recv.at[m, slot], (dev, me))

    def send_residual(m):
        for dx, dy in FAR_FIRST:
            s_copy(m, group_at(dx, dy), tm).start()
        srecv[m, tm] = yref[m, share(tm), :]

    def scan_groups():
        for m in range(2):
            cd = 1.0 / (1.0 + 2.0 * rsum[m, share(tm), :])
            corr = carried[m, share(tm), :]
            for d in range(1, TM):
                e = lax.rem(tm + d, TM)
                s_copy(m, e, e).wait_recv()
            for g in range(TM):
                corr = cd * corr + srecv[m, (g + TM - 1) % TM]
                ssend[m, (g + 1) % TM] = corr
            for dx, dy in FAR_FIRST:
                dest = group_at(dx, dy)
                c_copy(m, dest, dest, tm).start()
            crecv[m, tm] = ssend[m, tm]
        coef_shift.wait()
        for m in range(2):
            for d in range(1, TM):
                e = lax.rem(tm + d, TM)
                s_copy(m, e, tm).wait_send()
            for d in range(1, TM):
                e = lax.rem(tm + d, TM)
                c_copy(m, e, e, e).wait_recv()
            yref[m] = coefp[m] + crecv[m].reshape(B, M)
        for m in range(2):
            for d in range(1, TM):
                e = lax.rem(tm + d, TM)
                c_copy(m, e, e, tm).wait_send()

    def turn(k, carry):
        def left_rows(h, c):
            hi, lo = split(w[h, pl.ds(c * 4, 4)].reshape(2 * B, B).T)
            return hi, jnp.concatenate([hi, lo], axis=0)

        def left_part(h, rows, m, hi, both):
            cols = pl.ds(m * M, M)
            a = dot(both, uph[h, rows, cols])
            return a[:B] + a[B:] + dot(hi, upl[h, rows, cols])

        def waits(h, c):
            pl.when(k == 0)(lambda: wait_w(h, c, True))
            pl.when(k > 0)(lambda: wait_w(h, c, False))

        for n, (h, c) in enumerate(((0, 0), (0, 1), (1, 0), (1, 1))):
            waits(h, c)
            rows = pl.ds(c * 2 * B, 2 * B)
            hi, both = left_rows(h, c)
            for m in range(2):
                v = left_part(h, rows, m, hi, both)
                if n:
                    v += lacc[m]
                if n < 3:
                    lacc[m] = v
                else:
                    yref[m] = fd[m] * v
                    pl.when(k == 3)(lambda m=m: send_residual(m))
        pl.when(k == 0)(lambda: wait_w_sent(True))
        pl.when(k > 0)(lambda: wait_w_sent(False))

        @pl.when(k == 1)
        def _():
            coef[...] = yref[...]
            coef_shift.start()

        pl.when(k == 3)(scan_groups)

        for m in range(2):
            hi, lo = split(yref[m])
            yb[pl.ds(0, B), pl.ds(m * M, M)] = hi
            yb[pl.ds(B, B), pl.ds(m * M, M)] = lo

        for h in range(2):
            a = dot(yb[...], tph[h])
            v = a[:B] + a[B:] + dot(yb[pl.ds(0, B), :], tpl[h])
            sz[h] = v.T.reshape(SPACE, H, B)
            for c in range(2):
                for chip in chips:
                    unless_mine(chip, c, z_copy(h, mine, chip, c).start)
            z_in[h, mine] = sz[h, mine]

        for h in range(2):
            rows = rows_of(h)
            for c in range(2):
                for chip in chips:
                    unless_mine(chip, c, z_copy(h, c * 4 + chip, chip, c).wait_recv)
                depth = pl.ds(c * M, M)
                hi, lo = split(jnp.concatenate([z_in[h, c * 4 + i] for i in range(4)], axis=1))
                a = dot(jnp.concatenate([hi, lo], axis=0), th[depth, :])
                v = a[:H] + a[H:] + dot(hi, tl[depth, :])
                if c:
                    facc[rows, :] += v
                else:
                    facc[rows, :] = v

            @pl.when(k == 3)
            def _():
                csb[rows, :] = facc[rows, :]
                cs_shift[h].start()

            @pl.when(k < 4)
            def _():
                restart = ((k == 1) & (tm == TM - 1)) | ((k == 3) & (tm == 0))
                facc[rows, :] = react(jnp.where(restart, init[rows, :], facc[rows, :]))

                @pl.when(k == 0)
                def _():
                    nrf[rows, :] = facc[rows, :]
                    nrf_shift[h].start()
                    facc[rows, :] += fc[rows, :]

                @pl.when(k == 1)
                def _():
                    force_b[h].wait_send()
                    force_a[h].wait()
                    facc[rows, :] += ffn[rows, :]

                @pl.when(k == 2)
                def _():
                    nrf_shift[h].wait()
                    facc[rows, :] -= nrfn[rows, :]

                @pl.when(k == 3)
                def _():
                    facc[rows, :] += ff[rows, :]

                put_xs(h, facc[rows, :])
                right_send(h, False)

        for h in range(2):
            for c in range(2):
                for chip in chips:
                    unless_mine(chip, c, z_copy(h, mine, chip, c).wait_send)
        return carry

    lax.fori_loop(0, 5, turn, 0)
    fs_o[...] = facc[...]
    for h in range(2):
        guess_shift[h].wait_send()
        cs_shift[h].wait()


def on_device(initial_state, guess_coarse, force_fine, force_coarse, eigen_basis, eigen_rates, carried_correction):
    vm, dma = pltpu.VMEM, pltpu.SemaphoreType.DMA
    hbm = pl.BlockSpec(memory_space=pl.ANY)
    vmem = pl.BlockSpec(memory_space=pltpu.VMEM)
    field = vm((B, N), F32)
    column = vm((N, B), F32)
    blocks = vm((2, SPACE, H, B), F32)
    pair = vm((2, B, M), F32)
    shares = vm((2, TM, E, M), F32)
    basis = vm((N, N), BF16)
    two, eight, sixteen = dma((2,)), dma((2, SPACE)), dma((2, TM))
    fine, coarse = pl.pallas_call(
        kernel,
        out_shape=(jax.ShapeDtypeStruct((B, N), F32), jax.ShapeDtypeStruct((B, N), F32)),
        in_specs=[hbm] * 5 + [vmem, hbm],
        out_specs=(vmem, vmem),
        scratch_shapes=[
            vm((N, N), F32), basis, basis, basis, basis,
            vm((2, M, N), BF16), vm((2, M, N), BF16), vm((2, N, M), BF16), vm((2, N, M), BF16),
            field, field, field, field, column, pair,
            vm((2, Q, N), F32), field, field, field, pair, pair, field,
            blocks, blocks, blocks, blocks,
            vm((2, B, N), BF16), vm((2 * B, N), BF16),
            pair, pair, pair, pair, field, shares, shares, shares,
            dma((4,)), dma((5,)), two, two, two, two, two, two,
            two, two, dma, dma, two, two,
            eight, eight, eight, eight, eight, eight,
            sixteen, sixteen, sixteen, sixteen,
        ],
        compiler_params=pltpu.CompilerParams(
            collective_id=0, has_side_effects=True, vmem_limit_bytes=55000000
        ),
        name="mgrit_cycle",
    )(
        initial_state, guess_coarse[0], force_fine[0], force_coarse[0],
        eigen_basis, eigen_rates[None, :], carried_correction,
    )
    return fine[None], coarse[None]


def solution(mesh):
    rows = P("tm", "space", None)
    return jax.shard_map(
        on_device,
        mesh=mesh,
        in_specs=(P("space", None), rows, rows, rows, P(), P(), P()),
        out_specs=(rows, rows),
        check_vma=False,
    )
```

```python
import jax
import jax.numpy as jnp
from jax import lax
from jax.experimental import pallas as pl
from jax.experimental.pallas import tpu as pltpu
from jax.sharding import PartitionSpec as P

MESH = pl.DeviceIdType.MESH
F32 = jnp.float32
BF16 = jnp.bfloat16
TM = 16
SPACE = 8
N = 1024
B = 128
H = B // 2
Q = H // 2
R = Q // 2
M = N // 2
E = B // TM
FAR_FIRST = sorted(
    ((x, y) for x in range(4) for y in range(4) if x or y), key=lambda t: -min(t[0], 4 - t[0]) - min(t[1], 4 - t[1])
)


def dot(a, b):
    return jnp.dot(a, b, preferred_element_type=F32)


def react(field):
    return field + 0.5 * jnp.tanh(field)


def split(x):
    hi = x.astype(BF16)
    return hi, (x - hi.astype(F32)).astype(BF16)


def kernel(
    init_h, guess_h, ff_h, fc_h, u_h, rates, carried_h,
    fs_o, cs_o,
    ubuf, uh, ul, th, tl, uph, upl, tph, tpl, init, guess, ff, fc, cbuf, carried,
    ga, ffn, nrf, nrfn, coef, coefp, csb,
    sw, w, sz, z_in, xs, yb, fd, rsum, yref, lacc, facc, srecv, ssend, crecv,
    u_sem, loc_sem, ga_send, ga_recv, fb_send, fb_recv, fa_send, fa_recv,
    nr_send, nr_recv, co_send, co_recv, cs_send, cs_recv,
    w_send, w_recv, wb_send, wb_recv, z_send, z_recv,
    s_send, s_recv, c_send, c_recv,
):
    tm = lax.axis_index("tm")
    me = lax.axis_index("space")
    zc = me // 2
    core = me % 2
    mine = core * 4 + zc
    nxt = lax.rem(tm + 1, TM)
    prv = lax.rem(tm + TM - 1, TM)

    def remote(src, dst, ss, rs, dev):
        return pltpu.make_async_remote_copy(
            src_ref=src, dst_ref=dst, send_sem=ss, recv_sem=rs, device_id=dev, device_id_type=MESH
        )

    def chip_of(q):
        return lax.rem(zc + q, 4)

    chips = (chip_of(2), chip_of(1), chip_of(3), zc)

    def group_at(dx, dy):
        return lax.rem(tm // 4 + dx, 4) * 4 + lax.rem(tm % 4 + dy, 4)

    u_copies = [
        pltpu.make_async_copy(u_h.at[pl.ds(i * 256, 256)], ubuf.at[pl.ds(i * 256, 256)], u_sem.at[i])
        for i in range(4)
    ]
    own_cols = pl.ds(pl.multiple_of(me * B, B), B)
    loads = [
        pltpu.make_async_copy(init_h, init, loc_sem.at[0]),
        pltpu.make_async_copy(guess_h, guess, loc_sem.at[1]),
        pltpu.make_async_copy(ff_h, ff, loc_sem.at[2]),
        pltpu.make_async_copy(fc_h, fc, loc_sem.at[3]),
        pltpu.make_async_copy(carried_h.at[:, own_cols], cbuf, loc_sem.at[4]),
    ]
    for c in u_copies + loads:
        c.start()

    barrier = pltpu.get_barrier_semaphore()
    count = 0
    for d in range(1, SPACE):
        for t in (tm, nxt, prv):
            pl.semaphore_signal(barrier, inc=1, device_id=(t, lax.rem(me + d, SPACE)), device_id_type=MESH)
            count += 1
    for d in range(1, TM):
        pl.semaphore_signal(barrier, inc=1, device_id=(lax.rem(tm + d, TM), me), device_id_type=MESH)
        count += 1

    for c in loads:
        c.wait()
    pl.semaphore_wait(barrier, count)

    def part_a(i):
        return pl.ds(i * Q, R)

    def part_b(i):
        return pl.ds(i * Q + R, R)

    def rows_of(h):
        return pl.ds(h * H, H)

    guess_shift = [remote(guess.at[part_a(i)], ga.at[i], ga_send.at[i], ga_recv.at[i], (nxt, me)) for i in range(4)]
    force_b = [remote(ff.at[part_b(i)], ffn.at[part_b(i)], fb_send.at[i], fb_recv.at[i], (prv, me)) for i in range(4)]
    force_a = [remote(ff.at[part_a(i)], ffn.at[part_a(i)], fa_send.at[i], fa_recv.at[i], (prv, me)) for i in range(4)]
    nrf_shift = [remote(nrf.at[rows_of(h)], nrfn.at[rows_of(h)], nr_send.at[h], nr_recv.at[h], (prv, me)) for h in range(2)]
    coef_shift = remote(coef, coefp, co_send, co_recv, (nxt, me))
    cs_shift = [remote(csb.at[rows_of(h)], cs_o.at[rows_of(h)], cs_send.at[h], cs_recv.at[h], (prv, me)) for h in range(2)]
    for i in range(4):
        guess_shift[i].start()
        force_b[i].start()

    for c in u_copies:
        c.wait()

    def prep_natural(i, carry):
        at = pl.ds(pl.multiple_of(i * B, B), B)
        hi, lo = split(ubuf[at, :])
        for s in range(SPACE):
            old, new = slice(s * B, (s + 1) * B), pl.ds((s % 2 * 4 + s // 2) * B, B)
            uh[at, new] = hi[:, old]
            ul[at, new] = lo[:, old]
        hi, lo = split(ubuf[at, :].T)
        for s in range(SPACE):
            for p in range(2):
                old = slice(s * B + p * H, s * B + (p + 1) * H)
                new = pl.ds(p * M + (s % 2 * 4 + s // 2) * H, H)
                th[new, at] = hi[old]
                tl[new, at] = lo[old]
        return carry

    def prep_halves(j, carry):
        row = j % 4 // 2 * B + j // 4 * H + j % 2 * Q
        at = pl.ds(pl.multiple_of(j % 4 * B, B), B)
        x = jnp.concatenate([ubuf[pl.ds(pl.multiple_of(row + i * 2 * B, Q), Q), :] for i in range(4)], axis=0)
        hi, lo = split(x)
        uph[j // 4, at, :] = hi
        upl[j // 4, at, :] = lo
        hi, lo = split(x.T)
        tph[j // 4, :, at] = hi
        tpl[j // 4, :, at] = lo
        return carry

    lax.fori_loop(0, 8, prep_natural, 0)
    own = rates[:, own_cols]

    own_down = jnp.broadcast_to(own, (B, B)).T

    def prep_decay(i, carry):
        at = pl.ds(pl.multiple_of(i * B, B), B)
        half = pl.ds(pl.multiple_of(i % 4 * B, B), B)
        total = jnp.broadcast_to(rates[:, at], (B, B)) + own_down
        rates_in = 1.0 / (1.0 + total)
        before = cbuf[at, :].T
        for p in range(2):
            own_part = slice(p * H, (p + 1) * H)
            rsum[p, i // 4, :, half] = total[own_part]
            fd[p, i // 4, :, half] = rates_in[own_part]
            carried[p, i // 4, :, half] = before[own_part]
        return carry

    lax.fori_loop(0, 8, prep_decay, 0)

    keep, give = pl.ds(0, R), pl.ds(R, R)
    left = lax.broadcasted_iota(jnp.int32, (Q, B), 1) < H

    def w_copies(h, p, s, chip, c, first):
        d, dev, n = c * 4 + chip, chip * 2 + c, h * 2 + p
        if not first:
            return (remote(sw.at[n, d], w.at[n, s], w_send.at[n, d], w_recv.at[n, s], (tm, dev)),)
        return (
            remote(sw.at[n, d, keep], w.at[n, s, keep], w_send.at[n, d], w_recv.at[n, s], (tm, dev)),
            remote(sw.at[n, d, give], w.at[n, s, give], wb_send.at[n, d], wb_recv.at[n, s], (nxt, dev)),
        )

    def z_copy(h, p, s, chip, c):
        d, n = c * 4 + chip, h * 2 + p
        return remote(sz.at[n, d], z_in.at[n, s], z_send.at[n, d], z_recv.at[n, s], (tm, chip * 2 + c))

    def unless_mine(chip, c, act):
        if chip is zc:
            pl.when(core != c)(act)
        else:
            act()

    def w_start(h, p, c, first):
        for chip in chips:
            copies = w_copies(h, p, mine, chip, c, first)
            unless_mine(chip, c, copies[0].start)
            if first:
                copies[1].start()

    def right_send(h, first):
        for c in range(2):
            cols = pl.ds(c * M, M)
            a = dot(xs[h], uh[:, cols])
            p = a[:H] + a[H:] + dot(xs[h, pl.ds(0, H), :], ul[:, cols])
            for i in range(4):
                block = p[:, i * B:(i + 1) * B]
                turned = pltpu.roll(block, H, 1)
                sw[h * 2, c * 4 + i] = jnp.where(left, block[:Q], turned[Q:])
                sw[h * 2 + 1, c * 4 + i] = jnp.where(left, turned[:Q], block[Q:])
            for n in ((h, 0, c), (h, 1, c)) if h == 0 else ((h, 0, c),):
                w_start(*n, first)
        if h:
            for c in range(2):
                w_start(h, 1, c, first)
        for p in range(2):
            if first:
                w[h * 2 + p, mine, keep] = sw[h * 2 + p, mine, keep]
            else:
                w[h * 2 + p, mine] = sw[h * 2 + p, mine]

    def wait_w(h, p, c, first):
        for chip in chips:
            copies = w_copies(h, p, c * 4 + chip, chip, c, first)
            unless_mine(chip, c, copies[0].wait_recv)
            if first:
                copies[1].wait_recv()

    def wait_w_sent(first):
        for h in range(2):
            for p in range(2):
                for c in range(2):
                    for chip in chips:
                        copies = w_copies(h, p, mine, chip, c, first)
                        unless_mine(chip, c, copies[0].wait_send)
                        if first:
                            copies[1].wait_send()

    def put_xs(h, x):
        hi, lo = split(x)
        xs[h, pl.ds(0, H), :] = hi
        xs[h, pl.ds(H, H), :] = lo

    for h in range(2):
        x = []
        for i in (2 * h, 2 * h + 1):
            guess_shift[i].wait_recv()
            x.append(react(jnp.where(tm == 0, init[part_a(i), :], ga[i])) + ff[part_a(i), :])
            force_b[i].wait_recv()
            x.append(react(jnp.where(tm == TM - 1, init[part_b(i), :], guess[part_b(i), :])) + ffn[part_b(i), :])
        put_xs(h, jnp.concatenate(x, axis=0))
        right_send(h, True)
    for i in range(4):
        force_a[i].start()
    lax.fori_loop(0, 8, prep_halves, 0)

    def put_yb(p, m, y):
        hi, lo = split(y)
        yb[p, pl.ds(0, H), pl.ds(m * M, M)] = hi
        yb[p, pl.ds(H, H), pl.ds(m * M, M)] = lo

    def share(e):
        return pl.ds(pl.multiple_of(e // 2 * E, E), E)

    def s_copy(p, e, slot):
        return remote(yref.at[p, e % 2, share(e)], srecv.at[p, slot], s_send.at[p, e], s_recv.at[p, slot], (e, me))

    def c_copy(p, g, dev, slot):
        return remote(
            ssend.at[p, g], crecv.at[p, slot // 2, slot % 2], c_send.at[p, g], c_recv.at[p, slot], (dev, me)
        )

    def send_residual(p):
        for dx, dy in FAR_FIRST:
            s_copy(p, group_at(dx, dy), tm).start()
        srecv[p, tm] = yref[p, tm % 2, share(tm), :]

    def scan_groups():
        for p in range(2):
            cd = 1.0 / (1.0 + 2.0 * rsum[p, tm % 2, share(tm), :])
            corr = carried[p, tm % 2, share(tm), :]
            for d in range(1, TM):
                e = lax.rem(tm + d, TM)
                s_copy(p, e, e).wait_recv()
            for g in range(TM):
                corr = cd * corr + srecv[p, (g + TM - 1) % TM]
                ssend[p, (g + 1) % TM] = corr
            for dx, dy in FAR_FIRST:
                dest = group_at(dx, dy)
                c_copy(p, dest, dest, tm).start()
            crecv[p, tm // 2, tm % 2] = ssend[p, tm]
        coef_shift.wait()

    def take_correction(p):
        for d in range(1, TM):
            e = lax.rem(tm + d, TM)
            c_copy(p, e, e, e).wait_recv()
        for m in range(2):
            put_yb(p, m, coefp[p, m] + crecv[p, :, m].reshape(H, M))

    def scan_sent():
        for p in range(2):
            for d in range(1, TM):
                e = lax.rem(tm + d, TM)
                s_copy(p, e, tm).wait_send()
                c_copy(p, e, e, tm).wait_send()

    def left_inverse(h, p):
        a = dot(yb[p], tph[h])
        v = a[:H] + a[H:] + dot(yb[p, pl.ds(0, H), :], tpl[h])
        for c in range(2):
            at = c * 2 * B
            both = jnp.concatenate([v[:, at:at + B], v[:, at + B:at + 2 * B]], axis=0)
            sz[h * 2 + p, pl.ds(c * 4, 4)] = both.T.reshape(4, Q, B)
        z_start(h, p)

    def z_start(h, p):
        for c in range(2):
            for chip in chips:
                unless_mine(chip, c, z_copy(h, p, mine, chip, c).start)
        z_in[h * 2 + p, mine] = sz[h * 2 + p, mine]

    def turn(k, carry):
        def waits(h, p, c):
            pl.when(k == 0)(lambda: wait_w(h, p, c, True))
            pl.when(k > 0)(lambda: wait_w(h, p, c, False))

        def left_rows(h, p, c):
            t = w[h * 2 + p, pl.ds(c * 4, 4)].reshape(B, B).T
            return [t[:H], t[H:]]

        def left_part(h, rows, x):
            hi, lo = split(jnp.concatenate(x, axis=1))
            a = dot(jnp.concatenate([hi, lo], axis=0), uph[h, rows, :])
            return a[:H] + a[H:] + dot(hi, upl[h, rows, :])

        def finish(p):
            for c in range(2):
                waits(1, p, c)
                v = lacc[p] + left_part(1, pl.ds(c * 2 * B, 2 * B), left_rows(1, p, c))
                if c == 0:
                    lacc[p] = v
                else:
                    for m in range(2):
                        y = fd[p, m] * v[:, m * M:(m + 1) * M]
                        yref[p, m] = y
                        put_yb(p, m, y)

        for p in range(2):
            waits(0, p, 0)
            waits(0, p, 1)
            lacc[p] = left_part(0, pl.ds(0, M), left_rows(0, p, 0) + left_rows(0, p, 1))
        finish(0)
        pl.when(k == 3)(lambda: send_residual(0))
        pl.when(k != 3)(lambda: left_inverse(0, 0))
        finish(1)

        @pl.when(k == 3)
        def _():
            send_residual(1)
            scan_groups()
            take_correction(0)
            left_inverse(0, 0)
            take_correction(1)
            scan_sent()

        left_inverse(0, 1)
        left_inverse(1, 0)
        left_inverse(1, 1)

        pl.when(k == 0)(lambda: wait_w_sent(True))
        pl.when(k > 0)(lambda: wait_w_sent(False))

        @pl.when(k == 1)
        def _():
            coef[...] = yref[...]
            coef_shift.start()

        for h in range(2):
            rows = rows_of(h)
            for p in range(2):
                for c in range(2):
                    for chip in chips:
                        unless_mine(chip, c, z_copy(h, p, c * 4 + chip, chip, c).wait_recv)
                x = []
                for i in range(0, SPACE, 2):
                    one, two = z_in[h * 2 + p, i], z_in[h * 2 + p, i + 1]
                    x.append(jnp.concatenate(
                        [jnp.where(left, one, pltpu.roll(two, H, 1)), jnp.where(left, pltpu.roll(one, H, 1), two)], axis=0
                    ))
                depth = pl.ds(p * M, M)
                hi, lo = split(jnp.concatenate(x, axis=1))
                a = dot(jnp.concatenate([hi, lo], axis=0), th[depth, :])
                v = a[:H] + a[H:] + dot(hi, tl[depth, :])
                if p:
                    facc[rows, :] += v
                else:
                    facc[rows, :] = v

            @pl.when(k == 3)
            def _():
                csb[rows, :] = facc[rows, :]
                cs_shift[h].start()

            @pl.when(k < 4)
            def _():
                restart = ((k == 1) & (tm == TM - 1)) | ((k == 3) & (tm == 0))
                facc[rows, :] = react(jnp.where(restart, init[rows, :], facc[rows, :]))

                @pl.when(k == 0)
                def _():
                    nrf[rows, :] = facc[rows, :]
                    nrf_shift[h].start()
                    facc[rows, :] += fc[rows, :]

                @pl.when(k == 1)
                def _():
                    for i in (2 * h, 2 * h + 1):
                        force_b[i].wait_send()
                        force_a[i].wait()
                    facc[rows, :] += ffn[rows, :]

                @pl.when(k == 2)
                def _():
                    nrf_shift[h].wait()
                    facc[rows, :] -= nrfn[rows, :]

                @pl.when(k == 3)
                def _():
                    facc[rows, :] += ff[rows, :]

                put_xs(h, facc[rows, :])
                right_send(h, False)

        for h in range(2):
            for p in range(2):
                for c in range(2):
                    for chip in chips:
                        unless_mine(chip, c, z_copy(h, p, mine, chip, c).wait_send)
        return carry

    lax.fori_loop(0, 5, turn, 0)
    fs_o[...] = facc[...]
    for i in range(4):
        guess_shift[i].wait_send()
    for h in range(2):
        cs_shift[h].wait()


def on_device(initial_state, guess_coarse, force_fine, force_coarse, eigen_basis, eigen_rates, carried_correction):
    vm, dma = pltpu.VMEM, pltpu.SemaphoreType.DMA
    hbm = pl.BlockSpec(memory_space=pl.ANY)
    vmem = pl.BlockSpec(memory_space=pltpu.VMEM)
    field = vm((B, N), F32)
    column = vm((N, B), F32)
    blocks = vm((4, SPACE, Q, B), F32)
    pair = vm((2, 2, H, M), F32)
    shares = vm((2, TM, E, M), F32)
    basis = vm((N, N), BF16)
    two, four, eight, sixteen = dma((2,)), dma((4,)), dma((4, SPACE)), dma((2, TM))
    fine, coarse = pl.pallas_call(
        kernel,
        out_shape=(jax.ShapeDtypeStruct((B, N), F32), jax.ShapeDtypeStruct((B, N), F32)),
        in_specs=[hbm] * 5 + [vmem, hbm],
        out_specs=(vmem, vmem),
        scratch_shapes=[
            vm((N, N), F32), basis, basis, basis, basis,
            vm((2, M, N), BF16), vm((2, M, N), BF16), vm((2, N, M), BF16), vm((2, N, M), BF16),
            field, field, field, field, column, pair,
            vm((4, R, N), F32), field, field, field, pair, pair, field,
            blocks, blocks, blocks, blocks,
            vm((2, B, N), BF16), vm((2, B, N), BF16),
            pair, pair, pair, vm((2, H, N), F32), field, shares, shares, vm((2, TM // 2, 2, E, M), F32),
            dma((4,)), dma((5,)), four, four, four, four, four, four,
            two, two, dma, dma, two, two,
            eight, eight, eight, eight, eight, eight,
            sixteen, sixteen, sixteen, sixteen,
        ],
        compiler_params=pltpu.CompilerParams(
            collective_id=0, has_side_effects=True, vmem_limit_bytes=55000000
        ),
        name="mgrit_cycle",
    )(
        initial_state, guess_coarse[0], force_fine[0], force_coarse[0],
        eigen_basis, eigen_rates[None, :], carried_correction,
    )
    return fine[None], coarse[None]


def solution(mesh):
    rows = P("tm", "space", None)
    return jax.shard_map(
        on_device,
        mesh=mesh,
        in_specs=(P("space", None), rows, rows, rows, P(), P(), P()),
        out_specs=(rows, rows),
        check_vma=False,
    )
```

```python
import jax
import jax.numpy as jnp
from jax import lax
from jax.experimental import pallas as pl
from jax.experimental.pallas import tpu as pltpu
from jax.sharding import PartitionSpec as P

MESH = pl.DeviceIdType.MESH
F32 = jnp.float32
BF16 = jnp.bfloat16
TM = 16
SPACE = 8
N = 1024
B = 128
H = B // 2
Q = H // 2
R = Q // 2
M = N // 2
E = B // TM
FAR_FIRST = sorted(
    ((x, y) for x in range(4) for y in range(4) if x or y), key=lambda t: -min(t[0], 4 - t[0]) - min(t[1], 4 - t[1])
)


def dot(a, b):
    return jnp.dot(a, b, preferred_element_type=F32)


def react(field):
    return field + 0.5 * jnp.tanh(field)


def split(x):
    hi = x.astype(BF16)
    return hi, (x - hi.astype(F32)).astype(BF16)


def kernel(
    init_h, guess_h, ff_h, fc_h, u_h, rates, carried_h,
    fs_o, cs_o,
    ubuf, uh, ul, th, tl, uph, upl, tph, tpl, init, guess, ff, fc, cbuf, carried,
    ga, ffn, nrf, nrfn, coef, coefp, csb,
    sw, w, sz, z_in, xs, yb, fd, rsum, yref, lacc, facc, srecv, ssend, crecv,
    u_sem, loc_sem, ga_send, ga_recv, fb_send, fb_recv, fa_send, fa_recv,
    nr_send, nr_recv, co_send, co_recv, cs_send, cs_recv,
    w_send, w_recv, wb_send, wb_recv, z_send, z_recv,
    s_send, s_recv, c_send, c_recv, up_sem, down_sem,
):
    tm = lax.axis_index("tm")
    me = lax.axis_index("space")
    zc = me // 2
    core = me % 2
    mine = core * 4 + zc
    nxt = lax.rem(tm + 1, TM)
    prv = lax.rem(tm + TM - 1, TM)

    def remote(src, dst, ss, rs, dev):
        return pltpu.make_async_remote_copy(
            src_ref=src, dst_ref=dst, send_sem=ss, recv_sem=rs, device_id=dev, device_id_type=MESH
        )

    def chip_of(q):
        return lax.rem(zc + q, 4)

    chips = (chip_of(2), chip_of(1), chip_of(3), zc)

    def group_at(dx, dy):
        return lax.rem(tm // 4 + dx, 4) * 4 + lax.rem(tm % 4 + dy, 4)

    u_copies = [
        pltpu.make_async_copy(u_h.at[pl.ds(i * 256, 256)], ubuf.at[pl.ds(i * 256, 256)], u_sem.at[i])
        for i in range(4)
    ]
    own_cols = pl.ds(pl.multiple_of(me * B, B), B)
    loads = [
        pltpu.make_async_copy(init_h, init, loc_sem.at[0]),
        pltpu.make_async_copy(guess_h, guess, loc_sem.at[1]),
        pltpu.make_async_copy(ff_h, ff, loc_sem.at[2]),
        pltpu.make_async_copy(fc_h, fc, loc_sem.at[3]),
        pltpu.make_async_copy(carried_h.at[:, own_cols], cbuf, loc_sem.at[4]),
    ]
    for c in u_copies + loads:
        c.start()

    barrier = pltpu.get_barrier_semaphore()
    near = [(tm, lax.rem(me + d, SPACE)) for d in range(1, SPACE)] + [(nxt, me), (prv, me)]
    count = len(near)
    for dev in near:
        pl.semaphore_signal(barrier, inc=1, device_id=dev, device_id_type=MESH)

    for c in loads:
        c.wait()
    pl.semaphore_wait(barrier, count)

    def part_a(i):
        return pl.ds(i * Q, R)

    def part_b(i):
        return pl.ds(i * Q + R, R)

    def rows_of(h):
        return pl.ds(h * H, H)

    guess_shift = [remote(guess.at[part_a(i)], ga.at[i], ga_send.at[i], ga_recv.at[i], (nxt, me)) for i in range(4)]
    force_b = [remote(ff.at[part_b(i)], ffn.at[part_b(i)], fb_send.at[i], fb_recv.at[i], (prv, me)) for i in range(4)]
    force_a = [remote(ff.at[part_a(i)], ffn.at[part_a(i)], fa_send.at[i], fa_recv.at[i], (prv, me)) for i in range(4)]
    nrf_shift = [remote(nrf.at[rows_of(h)], nrfn.at[rows_of(h)], nr_send.at[h], nr_recv.at[h], (prv, me)) for h in range(2)]
    coef_shift = remote(coef, coefp, co_send, co_recv, (nxt, me))
    cs_shift = [remote(csb.at[rows_of(h)], cs_o.at[rows_of(h)], cs_send.at[h], cs_recv.at[h], (prv, me)) for h in range(2)]
    for i in range(4):
        guess_shift[i].start()
        force_b[i].start()

    for c in u_copies:
        c.wait()

    left_half = lax.broadcasted_iota(jnp.int32, (B, B), 1) < H

    def prep_natural(n, carry):
        at = pl.ds(pl.multiple_of(n * B, B), B)
        x = ubuf[at, :]
        for i in range(4):
            low = (i % 2 * 4 + i // 2) * B
            one, two = x[:, low:low + B], x[:, low + 2 * B:low + 3 * B]
            halves = (jnp.where(left_half, one, pltpu.roll(two, H, 1)), jnp.where(left_half, pltpu.roll(one, H, 1), two))
            for p in range(2):
                hi, lo = split(halves[p])
                uh[at, pl.ds(p * M + i * B, B)] = hi
                ul[at, pl.ds(p * M + i * B, B)] = lo
        hi, lo = split(ubuf[at, :].T)
        for s in range(SPACE):
            for p in range(2):
                old = slice(s * B + p * H, s * B + (p + 1) * H)
                new = pl.ds(p * M + (s % 2 * 4 + s // 2) * H, H)
                th[new, at] = hi[old]
                tl[new, at] = lo[old]
        return carry

    def prep_halves(j, carry):
        row = j % 4 // 2 * B + j // 4 * H + j % 2 * Q
        at = pl.ds(pl.multiple_of(j % 4 * B, B), B)
        x = jnp.concatenate([ubuf[pl.ds(pl.multiple_of(row + i * 2 * B, Q), Q), :] for i in range(4)], axis=0)
        hi, lo = split(x)
        uph[j // 4, at, :] = hi
        upl[j // 4, at, :] = lo
        hi, lo = split(x.T)
        tph[j // 4, :, at] = hi
        tpl[j // 4, :, at] = lo
        return carry

    lax.fori_loop(0, 8, prep_natural, 0)
    own = rates[:, own_cols]

    own_down = jnp.broadcast_to(own, (B, B)).T

    def prep_decay(i, carry):
        at = pl.ds(pl.multiple_of(i * B, B), B)
        half = pl.ds(pl.multiple_of(i % 4 * B, B), B)
        total = jnp.broadcast_to(rates[:, at], (B, B)) + own_down
        rates_in = 1.0 / (1.0 + total)
        before = cbuf[at, :].T
        for p in range(2):
            own_part = slice(p * H, (p + 1) * H)
            rsum[p, i // 4, :, half] = total[own_part]
            fd[p, i // 4, :, half] = rates_in[own_part]
            carried[p, i // 4, :, half] = before[own_part]
        return carry

    lax.fori_loop(0, 8, prep_decay, 0)

    keep, give = pl.ds(0, R), pl.ds(R, R)
    left = lax.broadcasted_iota(jnp.int32, (Q, B), 1) < H

    def w_copies(h, p, s, chip, c, first):
        d, dev, n = c * 4 + chip, chip * 2 + c, h * 2 + p
        if not first:
            return (remote(sw.at[n, d], w.at[n, s], w_send.at[n, d], w_recv.at[n, s], (tm, dev)),)
        return (
            remote(sw.at[n, d, keep], w.at[n, s, keep], w_send.at[n, d], w_recv.at[n, s], (tm, dev)),
            remote(sw.at[n, d, give], w.at[n, s, give], wb_send.at[n, d], wb_recv.at[n, s], (nxt, dev)),
        )

    def z_copy(h, p, s, chip, c):
        d, n = c * 4 + chip, h * 2 + p
        return remote(sz.at[n, d], z_in.at[n, s], z_send.at[n, d], z_recv.at[n, s], (tm, chip * 2 + c))

    def unless_mine(chip, c, act):
        if chip is zc:
            pl.when(core != c)(act)
        else:
            act()

    def w_start(h, p, c, first):
        for chip in chips:
            copies = w_copies(h, p, mine, chip, c, first)
            unless_mine(chip, c, copies[0].start)
            if first:
                copies[1].start()

    def right_send(h, first):
        for p in range(2):
            cols = pl.ds(p * M, M)
            a = dot(xs[h], uh[:, cols])
            x = a[:H] + a[H:] + dot(xs[h, pl.ds(0, H), :], ul[:, cols])
            for i in range(4):
                block = x[:, i * B:(i + 1) * B]
                turned = pltpu.roll(block, H, 1)
                sw[h * 2 + p, 2 * i] = jnp.where(left, block[:Q], turned[Q:])
                sw[h * 2 + p, 2 * i + 1] = jnp.where(left, turned[:Q], block[Q:])
            for c in range(2):
                w_start(h, p, c, first)
            if first:
                w[h * 2 + p, mine, keep] = sw[h * 2 + p, mine, keep]
            else:
                w[h * 2 + p, mine] = sw[h * 2 + p, mine]

    def wait_w(h, p, c, first):
        for chip in chips:
            copies = w_copies(h, p, c * 4 + chip, chip, c, first)
            unless_mine(chip, c, copies[0].wait_recv)
            if first:
                copies[1].wait_recv()

    def wait_w_sent(first):
        for h in range(2):
            for p in range(2):
                for c in range(2):
                    for chip in chips:
                        copies = w_copies(h, p, mine, chip, c, first)
                        unless_mine(chip, c, copies[0].wait_send)
                        if first:
                            copies[1].wait_send()

    def put_xs(h, x):
        hi, lo = split(x)
        xs[h, pl.ds(0, H), :] = hi
        xs[h, pl.ds(H, H), :] = lo

    for h in range(2):
        x = []
        for i in (2 * h, 2 * h + 1):
            guess_shift[i].wait_recv()
            x.append(react(jnp.where(tm == 0, init[part_a(i), :], ga[i])) + ff[part_a(i), :])
            force_b[i].wait_recv()
            x.append(react(jnp.where(tm == TM - 1, init[part_b(i), :], guess[part_b(i), :])) + ffn[part_b(i), :])
        put_xs(h, jnp.concatenate(x, axis=0))
        right_send(h, True)
    for i in range(4):
        force_a[i].start()
    lax.fori_loop(0, 8, prep_halves, 0)

    def put_yb(p, m, y):
        hi, lo = split(y)
        yb[p, pl.ds(0, H), pl.ds(m * M, M)] = hi
        yb[p, pl.ds(H, H), pl.ds(m * M, M)] = lo

    def share(e):
        return pl.ds(pl.multiple_of(e // 2 * E, E), E)

    def s_copy(p, e, slot):
        return remote(yref.at[p, e % 2, share(e)], srecv.at[p, slot], s_send.at[p, e], s_recv.at[p, slot], (e, me))

    def c_copy(p, g, dev, slot):
        return remote(
            ssend.at[p, g], crecv.at[p, slot // 2, slot % 2], c_send.at[p, g], c_recv.at[p, slot], (dev, me)
        )

    def send_residual(p):
        for dx, dy in FAR_FIRST:
            s_copy(p, group_at(dx, dy), tm).start()
        srecv[p, tm] = yref[p, tm % 2, share(tm), :]

    def scan_groups():
        for p in range(2):
            cd = 1.0 / (1.0 + 2.0 * rsum[p, tm % 2, share(tm), :])
            corr = carried[p, tm % 2, share(tm), :]
            for d in range(1, TM):
                e = lax.rem(tm + d, TM)
                s_copy(p, e, e).wait_recv()
            for g in range(TM):
                corr = cd * corr + srecv[p, (g + TM - 1) % TM]
                ssend[p, (g + 1) % TM] = corr
            for dx, dy in FAR_FIRST:
                dest = group_at(dx, dy)
                c_copy(p, dest, dest, tm).start()
            crecv[p, tm // 2, tm % 2] = ssend[p, tm]
        coef_shift.wait()

    def take_correction(p):
        for d in range(1, TM):
            e = lax.rem(tm + d, TM)
            c_copy(p, e, e, e).wait_recv()
        for m in range(2):
            put_yb(p, m, coefp[p, m] + crecv[p, :, m].reshape(H, M))

    def scan_sent():
        for p in range(2):
            for d in range(1, TM):
                e = lax.rem(tm + d, TM)
                s_copy(p, e, tm).wait_send()
                c_copy(p, e, e, tm).wait_send()

    def left_inverse(h, p):
        a = dot(yb[p], tph[h])
        v = a[:H] + a[H:] + dot(yb[p, pl.ds(0, H), :], tpl[h])
        for c in range(2):
            at = c * 2 * B
            both = jnp.concatenate([v[:, at:at + B], v[:, at + B:at + 2 * B]], axis=0)
            sz[h * 2 + p, pl.ds(c * 4, 4)] = both.T.reshape(4, Q, B)
        z_start(h, p)

    def z_start(h, p):
        for c in range(2):
            for chip in chips:
                unless_mine(chip, c, z_copy(h, p, mine, chip, c).start)
        z_in[h * 2 + p, mine] = sz[h * 2 + p, mine]

    def hear():
        pl.semaphore_wait(up_sem, 1)
        pl.semaphore_wait(down_sem, 1)

    def pass_word(k, place):
        @pl.when(k < 3)
        def _():
            if place:
                hear()
            else:
                pl.when(k > 0)(hear)
            pl.semaphore_signal(up_sem, inc=1, device_id=(nxt, me), device_id_type=MESH)
            pl.semaphore_signal(down_sem, inc=1, device_id=(prv, me), device_id_type=MESH)

    def turn(k, carry):
        pass_word(k, 0)
        def waits(h, p, c):
            pl.when(k == 0)(lambda: wait_w(h, p, c, True))
            pl.when(k > 0)(lambda: wait_w(h, p, c, False))

        def left_rows(h, p, c):
            t = w[h * 2 + p, pl.ds(c * 4, 4)].reshape(B, B).T
            return [t[:H], t[H:]]

        def left_part(h, rows, x):
            hi, lo = split(jnp.concatenate(x, axis=1))
            a = dot(jnp.concatenate([hi, lo], axis=0), uph[h, rows, :])
            return a[:H] + a[H:] + dot(hi, upl[h, rows, :])

        def finish(p):
            for c in range(2):
                waits(1, p, c)
                v = lacc[p] + left_part(1, pl.ds(c * 2 * B, 2 * B), left_rows(1, p, c))
                if c == 0:
                    lacc[p] = v
                else:
                    for m in range(2):
                        y = fd[p, m] * v[:, m * M:(m + 1) * M]
                        yref[p, m] = y
                        put_yb(p, m, y)

        for p in range(2):
            waits(0, p, 0)
            waits(0, p, 1)
            lacc[p] = left_part(0, pl.ds(0, M), left_rows(0, p, 0) + left_rows(0, p, 1))
        finish(0)
        @pl.when(k == 3)
        def _():
            hear()
            send_residual(0)

        pl.when(k != 3)(lambda: left_inverse(0, 0))
        finish(1)

        @pl.when(k == 3)
        def _():
            send_residual(1)
            scan_groups()
            take_correction(0)
            left_inverse(0, 0)
            take_correction(1)
            scan_sent()

        left_inverse(0, 1)
        left_inverse(1, 0)
        left_inverse(1, 1)

        pass_word(k, 1)
        pl.when(k == 0)(lambda: wait_w_sent(True))
        pl.when(k > 0)(lambda: wait_w_sent(False))

        @pl.when(k == 1)
        def _():
            coef[...] = yref[...]
            coef_shift.start()

        for h in range(2):
            if h:
                pass_word(k, 2)
            rows = rows_of(h)
            for p in range(2):
                for c in range(2):
                    for chip in chips:
                        unless_mine(chip, c, z_copy(h, p, c * 4 + chip, chip, c).wait_recv)
                x = []
                for i in range(0, SPACE, 2):
                    one, two = z_in[h * 2 + p, i], z_in[h * 2 + p, i + 1]
                    x.append(jnp.concatenate(
                        [jnp.where(left, one, pltpu.roll(two, H, 1)), jnp.where(left, pltpu.roll(one, H, 1), two)], axis=0
                    ))
                depth = pl.ds(p * M, M)
                hi, lo = split(jnp.concatenate(x, axis=1))
                a = dot(jnp.concatenate([hi, lo], axis=0), th[depth, :])
                v = a[:H] + a[H:] + dot(hi, tl[depth, :])
                if p:
                    facc[rows, :] += v
                else:
                    facc[rows, :] = v

            @pl.when(k == 3)
            def _():
                csb[rows, :] = facc[rows, :]
                cs_shift[h].start()

            @pl.when(k < 4)
            def _():
                restart = ((k == 1) & (tm == TM - 1)) | ((k == 3) & (tm == 0))
                facc[rows, :] = react(jnp.where(restart, init[rows, :], facc[rows, :]))

                @pl.when(k == 0)
                def _():
                    nrf[rows, :] = facc[rows, :]
                    nrf_shift[h].start()
                    facc[rows, :] += fc[rows, :]

                @pl.when(k == 1)
                def _():
                    for i in (2 * h, 2 * h + 1):
                        force_b[i].wait_send()
                        force_a[i].wait()
                    facc[rows, :] += ffn[rows, :]

                @pl.when(k == 2)
                def _():
                    nrf_shift[h].wait()
                    facc[rows, :] -= nrfn[rows, :]

                @pl.when(k == 3)
                def _():
                    facc[rows, :] += ff[rows, :]

                put_xs(h, facc[rows, :])
                right_send(h, False)

        for h in range(2):
            for p in range(2):
                for c in range(2):
                    for chip in chips:
                        unless_mine(chip, c, z_copy(h, p, mine, chip, c).wait_send)
        return carry

    lax.fori_loop(0, 5, turn, 0)
    fs_o[...] = facc[...]
    for i in range(4):
        guess_shift[i].wait_send()
    for h in range(2):
        cs_shift[h].wait()


def on_device(initial_state, guess_coarse, force_fine, force_coarse, eigen_basis, eigen_rates, carried_correction):
    vm, dma = pltpu.VMEM, pltpu.SemaphoreType.DMA
    hbm = pl.BlockSpec(memory_space=pl.ANY)
    vmem = pl.BlockSpec(memory_space=pltpu.VMEM)
    field = vm((B, N), F32)
    column = vm((N, B), F32)
    blocks = vm((4, SPACE, Q, B), F32)
    pair = vm((2, 2, H, M), F32)
    shares = vm((2, TM, E, M), F32)
    basis = vm((N, N), BF16)
    two, four, eight, sixteen = dma((2,)), dma((4,)), dma((4, SPACE)), dma((2, TM))
    fine, coarse = pl.pallas_call(
        kernel,
        out_shape=(jax.ShapeDtypeStruct((B, N), F32), jax.ShapeDtypeStruct((B, N), F32)),
        in_specs=[hbm] * 5 + [vmem, hbm],
        out_specs=(vmem, vmem),
        scratch_shapes=[
            vm((N, N), F32), basis, basis, basis, basis,
            vm((2, M, N), BF16), vm((2, M, N), BF16), vm((2, N, M), BF16), vm((2, N, M), BF16),
            field, field, field, field, column, pair,
            vm((4, R, N), F32), field, field, field, pair, pair, field,
            blocks, blocks, blocks, blocks,
            vm((2, B, N), BF16), vm((2, B, N), BF16),
            pair, pair, pair, vm((2, H, N), F32), field, shares, shares, vm((2, TM // 2, 2, E, M), F32),
            dma((4,)), dma((5,)), four, four, four, four, four, four,
            two, two, dma, dma, two, two,
            eight, eight, eight, eight, eight, eight,
            sixteen, sixteen, sixteen, sixteen, pltpu.SemaphoreType.REGULAR, pltpu.SemaphoreType.REGULAR,
        ],
        compiler_params=pltpu.CompilerParams(
            collective_id=0, has_side_effects=True, vmem_limit_bytes=55000000
        ),
        name="mgrit_cycle",
    )(
        initial_state, guess_coarse[0], force_fine[0], force_coarse[0],
        eigen_basis, eigen_rates[None, :], carried_correction,
    )
    return fine[None], coarse[None]


def solution(mesh):
    rows = P("tm", "space", None)
    return jax.shard_map(
        on_device,
        mesh=mesh,
        in_specs=(P("space", None), rows, rows, rows, P(), P(), P()),
        out_specs=(rows, rows),
        check_vma=False,
    )
```
